512 devices in a mesh: batch: 16 (over y, x), ctx: 32 (over z, core).
Axes of the slice: x: 4, y: 4, z: 16, core: 2. Of those that a mesh axis runs over, the one named last changes fastest.
Arguments:
- asked_for: bfloat16 [16, 4096, 64, 64], P('batch', 'ctx'), may hold values from -6 to 6
- offered: bfloat16 [16, 4096, 64, 64], P('batch', 'ctx'), may hold values from -6 to 6
- contents: bfloat16 [16, 4096, 64, 64], P('batch', 'ctx'), may hold values from -6 to 6
- out_weight: bfloat16 [4096, 4096], P('batch'), may hold values from -0.09375 to 0.09375
Outputs:
- layer_out: bfloat16 [16, 4096, 4096], P('batch', 'ctx')
The draws below stay inside these ranges and needn't reach their ends.
All inputs are finite; a program needn't handle non-finite values.
Results may differ from the reference program's by a relative error of at most 0.006.
Values may be sent and summed in bfloat16 or wider, within the bound.
A program may use at most 128 MiB of HBM per device.

```python
import jax
import jax.numpy as jnp
from jax import lax

HEADS = 64
HEAD_SIZE = 64
BATCH = 16
TOKENS = 4096
WIDTH = 4096


def shard_levels(key, dims, split, least, top_value):
    level = 1.0
    for axis_at, shards_of in split:
        steps = jax.random.uniform(jax.random.fold_in(jax.random.fold_in(key, 6), axis_at), (shards_of,), jnp.float32, least / len(split), top_value / len(split))
        level = level * jnp.repeat(jnp.exp(steps), dims[axis_at] // shards_of).reshape((-1,) + (1,) * (len(dims) - 1 - axis_at))
    return level


def centred(rng, extent, width, bound, pieces=(), kind=jnp.bfloat16):
    entries = jax.random.normal(rng, extent, jnp.float32) * width
    if len(pieces) > 0:
        entries = shard_levels(rng, extent, pieces, -0.22, 0.18) * entries
    return jnp.clip(entries, min=-bound, max=bound).astype(kind)


def setup_inputs(seed: int = 0) -> dict:
    key_of = jax.random.split(jax.random.key(seed), 5)
    return {
        "asked_for": centred(key_of[0], (BATCH, TOKENS, HEADS, HEAD_SIZE), 1.0, 6.0, ((0, 16), (1, 32))),
        "offered": centred(key_of[1], (BATCH, TOKENS, HEADS, HEAD_SIZE), 1.0, 6.0, ((0, 16), (1, 32))),
        "contents": centred(key_of[2], (BATCH, TOKENS, HEADS, HEAD_SIZE), 1.0, 6.0, ((0, 16), (1, 32))),
        "out_weight": centred(key_of[3], (WIDTH, WIDTH), WIDTH ** -0.5, 0.09375, ((0, 16),)),
    }


def to_features(values):
    wide = values.astype(jnp.float32)
    return (jax.nn.softplus(wide)).astype(jnp.bfloat16)


def after_reading(read, count):
    result = read * count ** 0.5
    return result.astype(jnp.bfloat16)


def look_up(features, state, mass):
    small = lax.optimization_barrier(state.astype(jnp.bfloat16))
    top = jnp.einsum("bthd,bhde->bthe", features.astype(jnp.float32), small.astype(jnp.float32))
    bottom = jnp.einsum("bthd,bhd->bth", features.astype(jnp.float32), mass, precision=lax.Precision.HIGHEST)
    return top / (bottom + 1e-3)[..., None]


def reference(asked_for, offered, contents, out_weight):
    query_feature, key_feature = lax.optimization_barrier((to_features(asked_for), to_features(offered)))
    state = jnp.einsum("bthd,bthe->bhde", key_feature.astype(jnp.float32), contents.astype(jnp.float32)) / TOKENS
    mass = jnp.sum(key_feature.astype(jnp.float32), axis=1) / TOKENS
    mixed = after_reading(look_up(query_feature, state, mass), TOKENS).reshape(BATCH, TOKENS, WIDTH)
    mixed = lax.optimization_barrier(mixed)
    layer_out = jnp.einsum("btw,wv->btv", mixed.astype(jnp.float32), out_weight.astype(jnp.float32)).astype(jnp.bfloat16)
    return layer_out
```

```python
import jax
import jax.numpy as jnp
from jax import lax
from jax.experimental import pallas as pl
from jax.experimental.pallas import tpu as pltpu
from jax.sharding import PartitionSpec as P

BF = jnp.bfloat16
F32 = jnp.float32
MESH = pl.DeviceIdType.MESH
D = 4096
T = 128
NC = 4
CW = 256
SR = 80
QP = 8


def feature(x):
    return jnp.log(1.0 + jnp.exp(x.astype(F32))).astype(BF)


def pack(s):
    m = s[64:72]
    hi = m.astype(BF).astype(F32)
    return jnp.concatenate([s[0:64], hi, m - hi], axis=0).astype(BF)


def unpack(b):
    f = b.astype(F32)
    m = f[64:72] + f[72:80]
    return jnp.concatenate([f[0:64], m, m], axis=0)


def kernel(
    q_hbm, k_hbm, v_hbm, w_hbm, out_ref,
    wbuf, qbuf, kbuf, vbuf, qf, st, dsend, drecv, r1s, r1r, acc, r2s, r2r, gat, mixed, obuf,
    lsem, w_ss, w_rs, q_ss, q_rs, d_ss, d_rs, r1_ss, r1_rs, r2_ss, r2_rs, g2_ss, g2_rs, g1_ss, g1_rs,
    gd_ss, gd_rs, o_ss, o_rs, semA, semB,
):
    b = lax.axis_index("batch")
    t = lax.axis_index("ctx")
    y, x = b // 4, b % 4
    z, core = t // 2, t % 2
    zp = z % 2
    me = 2 * zp + core
    sib = 2 * zp + (1 - core)
    zo = z + 1 - 2 * zp
    cls, m0 = z % 4, z // 4

    def dev(dy=0, dx=0, zz=None, cc=None):
        zz = z if zz is None else zz
        cc = core if cc is None else cc
        return (((y + dy) % 4) * 4 + (x + dx) % 4, zz * 2 + cc)

    def zdev(dz):
        return dev(zz=(z + dz + 16) % 16)

    lw = [
        pltpu.make_async_copy(
            w_hbm.at[:, pl.ds(pl.multiple_of(me * (NC * CW) + c * CW, CW), CW)],
            wbuf.at[c, pl.ds(pl.multiple_of(b * 256, 256), 256), :],
            lsem.at[c],
        )
        for c in range(NC)
    ]
    lk = pltpu.make_async_copy(k_hbm, kbuf, lsem.at[NC])
    lv = pltpu.make_async_copy(v_hbm, vbuf, lsem.at[NC + 1])
    lq = pltpu.make_async_copy(q_hbm, qbuf.at[me], lsem.at[NC + 2])
    for c in lw + [lk, lv, lq]:
        c.start()

    barrier = pltpu.get_barrier_semaphore()
    near = [
        dev(dx=1), dev(dx=3), dev(dy=1), dev(dy=3), dev(cc=1 - core),
        zdev(1), zdev(-1), zdev(2), zdev(-2), dev(zz=zo, cc=1 - core),
    ]
    for d in near:
        pl.semaphore_signal(barrier, inc=1, device_id=d, device_id_type=MESH)
    pl.semaphore_wait(barrier, len(near))
    for d in (zdev(2), zdev(-2)):
        pl.semaphore_signal(semA, inc=1, device_id=d, device_id_type=MESH)

    def wcopy(c, h, dy, dx, ty=0, tx=0):
        blk = ((y + dy) % 4) * 4 + (x + dx) % 4
        ref = wbuf.at[c, pl.ds(pl.multiple_of(blk * 256 + h * 128, 128), 128), :]
        return pltpu.make_async_remote_copy(
            src_ref=ref, dst_ref=ref, send_sem=w_ss,
            recv_sem=w_rs.at[c, h, ((dy - ty) % 4) * 4 + (dx - tx) % 4],
            device_id=dev(dy=ty % 4, dx=tx % 4), device_id_type=MESH,
        )

    def wd(h, dp, ds):
        return (ds % 4, dp % 4) if h == 0 else (dp % 4, ds % 4)

    def wsend(c, h, dp, ds, tp, ts):
        wcopy(c, h, *wd(h, dp, ds), *wd(h, tp, ts)).start()

    def wwait(c, h, dp, ds):
        wcopy(c, h, *wd(h, dp, ds)).wait_recv()

    def e0(c):
        for h in (0, 1):
            for tp, ts in ((1, 0), (-1, 0), (0, 1), (0, -1)):
                wsend(c, h, 0, 0, tp, ts)

    def e1(c):
        for h in (0, 1):
            wwait(c, h, -1, 0)
            if c % 2 == 0:
                wsend(c, h, -1, 0, 1, 0)
            wsend(c, h, -1, 0, 0, 1)
            wsend(c, h, -1, 0, 0, -1)
            wwait(c, h, 1, 0)
            if c % 2 == 1:
                wsend(c, h, 1, 0, -1, 0)
            wsend(c, h, 1, 0, 0, 1)
            wsend(c, h, 1, 0, 0, -1)

    def e3(c):
        for h in (0, 1):
            wwait(c, h, 2, 0)
            wsend(c, h, 2, 0, 0, 1)
            wsend(c, h, 2, 0, 0, -1)

    def e4(c):
        for h in (0, 1):
            for dp, ds in ((0, -1), (-1, 1), (1, -1), (2, 1)):
                wwait(c, h, dp, ds)
                wsend(c, h, dp, ds, 0, -ds)

    def e5(c):
        for h in (0, 1):
            for dp, ds in ((0, 1), (1, 1), (-1, -1), (2, -1), (0, 2), (1, 2), (-1, 2), (2, 2)):
                wwait(c, h, dp, ds)

    qr = D // QP

    def qcopy(slot, i, n, target, path):
        ref = qbuf.at[slot, pl.ds(i * qr, n * qr), :]
        return pltpu.make_async_remote_copy(
            src_ref=ref, dst_ref=ref, send_sem=q_ss, recv_sem=q_rs.at[path, i], device_id=target, device_id_type=MESH
        )

    zs = 2 * (1 - zp) + core
    zs2 = 2 * (1 - zp) + (1 - core)

    def qlink(lo, hi):
        for i in range(lo, hi):
            qcopy(me, i, 1, dev(zz=zo), 1).start()

    def qrelay(lo, hi):
        for i in range(lo, hi):
            qcopy(zs, i, 1, dev(zz=zo), 1).wait_recv()
            qcopy(zs, i, 1, dev(cc=1 - core), 2).start()

    def qfeat(slot, lo, hi):
        def body(i, _):
            r = pl.ds(pl.multiple_of(i * 128, 128), 128)
            qf[slot, r, :] = feature(qbuf[slot, r, :])
            return 0
        lax.fori_loop(lo * (32 // QP), hi * (32 // QP), body, 0)

    for c in range(NC):
        lw[c].wait()
        e0(c)
    lq.wait()
    qcopy(me, 0, QP, dev(cc=1 - core), 0).start()
    qlink(0, 2)

    lk.wait()
    lv.wait()
    lane = lax.broadcasted_iota(jnp.int32, (64, 128), 1) < 64
    ones = jnp.ones((16, 128), BF)
    nt = (((1,), (1,)), ((), ()))

    def partial(half, i):
        k, m = i // 4, i % 4
        r = pl.ds(pl.multiple_of((16 * half + 4 * m + k) * 128, 128), 128)
        kf = feature(kbuf[r, :])
        g = lax.dot_general(vbuf[r, :], kf, nt, preferred_element_type=F32)
        n = lax.dot_general(ones, kf, nt, preferred_element_type=F32)
        return k, m, jnp.concatenate([jnp.where(lane, g[0:64], g[64:128]), n], axis=0)

    def theirs(i, _):
        k, m, s = partial(1 - core, i)
        dsend[k, m] = pack(s)
        return 0

    def mine(i, _):
        k, m, s = partial(core, i)
        st[k, m] = s
        return 0

    lax.fori_loop(0, 16, theirs, 0)
    dcopy = pltpu.make_async_remote_copy(
        src_ref=dsend, dst_ref=drecv, send_sem=d_ss, recv_sem=d_rs, device_id=dev(cc=1 - core), device_id_type=MESH
    )
    dcopy.start()
    lax.fori_loop(0, 16, mine, 0)
    e1(0)
    dcopy.wait_recv()

    def chip_sum(i, _):
        k, m = i // 4, i % 4
        s = st[k, m] + unpack(drecv[k, m])
        st[k, m] = s
        r1s[k, m] = pack(s)
        return 0

    lax.fori_loop(0, 16, chip_sum, 0)

    def r1copy(n):
        dz, slot, lo, cnt = ((1, 0, 0, 4), (-1, 1, 0, 4), (2, 2, 0, 2), (-2, 2, 2, 2))[n]
        k = (z + dz + 16) % 4
        return pltpu.make_async_remote_copy(
            src_ref=r1s.at[k, pl.ds(lo, cnt)], dst_ref=r1r.at[slot, pl.ds(lo, cnt)],
            send_sem=r1_ss.at[n], recv_sem=r1_rs.at[n], device_id=zdev(dz), device_id_type=MESH,
        )

    for n in (2, 3, 0, 1):
        r1copy(n).start()
    qlink(2, 4)
    e1(1)
    pl.semaphore_wait(semA, 2)
    for d in (zdev(4), zdev(-4)):
        pl.semaphore_signal(semB, inc=1, device_id=d, device_id_type=MESH)
    qfeat(me, 0, QP)
    e1(2)
    for n in (0, 1, 2, 3):
        r1copy(n).wait_recv()

    def near_sum(m, _):
        s = st[cls, m] + unpack(r1r[0, m]) + unpack(r1r[1, m]) + unpack(r1r[2, m])
        acc[m] = s
        r2s[m] = pack(s)
        return 0

    lax.fori_loop(0, 4, near_sum, 0)

    def r2copy(r):
        return pltpu.make_async_remote_copy(
            src_ref=r2s.at[(m0 + r) % 4], dst_ref=r2r.at[r - 1],
            send_sem=r2_ss.at[r - 1], recv_sem=r2_rs.at[r - 1], device_id=zdev(4 * r), device_id_type=MESH,
        )

    pl.semaphore_wait(semB, 2)
    for r in (2, 1, 3):
        r2copy(r).start()
    qlink(4, 8)
    e1(3)
    qcopy(me, 0, QP, dev(cc=1 - core), 0).wait_recv()
    qfeat(sib, 0, QP)
    for c in range(NC):
        e3(c)
    qrelay(0, 4)
    for r in (1, 2, 3):
        r2copy(r).wait_recv()
    total = (acc[m0] + unpack(r2r[0]) + unpack(r2r[1]) + unpack(r2r[2])) * (1.0 / 4096.0)
    gat[core, cls, m0] = pack(total)

    def g2copy(r):
        ref = gat.at[core, cls, m0]
        return pltpu.make_async_remote_copy(
            src_ref=ref, dst_ref=ref, send_sem=g2_ss.at[r - 1], recv_sem=g2_rs.at[r - 1],
            device_id=zdev(4 * r), device_id_type=MESH,
        )

    for r in (2, 1, 3):
        g2copy(r).start()
    e4(0)
    qrelay(4, 8)
    qfeat(zs, 0, QP)
    e4(1)
    for r in (1, 2, 3):
        g2copy(r).wait_recv()

    def g1copy(n):
        dz, lo, cnt = ((1, 0, 4), (-1, 0, 4), (2, 0, 2), (-2, 2, 2))[n]
        ref = gat.at[core, cls, pl.ds(lo, cnt)]
        return pltpu.make_async_remote_copy(
            src_ref=ref, dst_ref=ref, send_sem=g1_ss.at[n], recv_sem=g1_rs.at[n],
            device_id=zdev(dz), device_id_type=MESH,
        )

    def gdcopy(dk):
        ref = gat.at[core, (cls + dk) % 4]
        return pltpu.make_async_remote_copy(
            src_ref=ref, dst_ref=ref, send_sem=gd_ss.at[dk], recv_sem=gd_rs.at[dk],
            device_id=dev(cc=1 - core), device_id_type=MESH,
        )

    for n in (2, 3, 0, 1):
        g1copy(n).start()
    gdcopy(0).start()
    e4(2)
    for i in range(QP):
        qcopy(zs2, i, 1, dev(cc=1 - core), 2).wait_recv()
    qfeat(zs2, 0, QP)
    g1copy(0).wait_recv()
    gdcopy(3).start()
    g1copy(1).wait_recv()
    gdcopy(1).start()
    g1copy(2).wait_recv()
    g1copy(3).wait_recv()
    gdcopy(2).start()
    e4(3)

    def mix(half, i):
        k, m = i // 4, i % 4
        pair = 16 * half + 4 * m + k
        r = pl.ds(pl.multiple_of(pair * 128, 128), 128)
        s = gat[half, k, m].astype(F32)
        a, n = s[0:64], s[64:80]
        lo16 = lane[0:16]
        lhs = jnp.concatenate(
            [jnp.where(lane, a, 0.0), jnp.where(lane, 0.0, a), jnp.where(lo16, n, 0.0), jnp.where(lo16, 0.0, n)], axis=0
        ).astype(BF)
        rhs = jnp.concatenate([qf[u, r, :] for u in range(4)], axis=1)
        g = jnp.dot(lhs, rhs, preferred_element_type=F32)
        r0 = 64.0 / (g[128:129] + g[136:137] + 1e-3)
        r1 = 64.0 / (g[144:145] + g[152:153] + 1e-3)
        got = jnp.concatenate([g[0:64] * r0, g[64:128] * r1], axis=0).astype(BF)
        mixed[:, r] = got.T

    lax.fori_loop(0, 16, lambda i, _: (mix(core, i), 0)[1], 0)
    for dk in range(4):
        gdcopy(dk).wait_recv()
    lax.fori_loop(0, 16, lambda i, _: (mix(1 - core, i), 0)[1], 0)

    def ocopy(c, r):
        s = (me + r) % 4
        return pltpu.make_async_remote_copy(
            src_ref=obuf.at[c, pl.ds(pl.multiple_of(s * T, T), T), :],
            dst_ref=out_ref.at[:, pl.ds(pl.multiple_of(me * (NC * CW) + c * CW, CW), CW)],
            send_sem=o_ss.at[c, r - 1], recv_sem=o_rs.at[c, r - 1],
            device_id=dev(zz=z - zp + s // 2, cc=s % 2), device_id_type=MESH,
        )

    for c in range(NC):
        e5(c)
        got = jnp.dot(mixed[...], wbuf[c], preferred_element_type=F32)
        obuf[c] = got.astype(BF)
        for r in (2, 1, 3):
            ocopy(c, r).start()
        out_ref[:, pl.ds(pl.multiple_of(me * (NC * CW) + c * CW, CW), CW)] = obuf[c, pl.ds(pl.multiple_of(me * T, T), T), :]

    for c in range(NC):
        for r in (1, 2, 3):
            ocopy(c, r).wait_recv()
    for c in range(NC):
        for r in (1, 2, 3):
            ocopy(c, r).wait_send()
    dcopy.wait_send()
    for n in range(4):
        r1copy(n).wait_send()
        g1copy(n).wait_send()
        gdcopy(n).wait_send()
    for r in (1, 2, 3):
        r2copy(r).wait_send()
        g2copy(r).wait_send()
    wref = wbuf.at[:, pl.ds(0, 3840), :]
    pltpu.make_async_copy(wref, wref, w_ss).wait()
    qref = qbuf.at[pl.ds(0, 3)]
    pltpu.make_async_copy(qref, qref, q_ss).wait()


def shards(asked_for, offered, contents, out_weight):
    def view(a):
        return jnp.transpose(a, (0, 2, 3, 1)).reshape(D, T)

    dma = pltpu.SemaphoreType.DMA
    hbm = pl.BlockSpec(memory_space=pl.ANY)
    out = pl.pallas_call(
        kernel,
        out_shape=jax.ShapeDtypeStruct((T, D), BF),
        in_specs=[hbm] * 4,
        out_specs=pl.BlockSpec(memory_space=pltpu.VMEM),
        scratch_shapes=[
            pltpu.VMEM((NC, D, CW), BF),
            pltpu.VMEM((4, D, T), BF),
            pltpu.VMEM((D, T), BF),
            pltpu.VMEM((D, T), BF),
            pltpu.VMEM((4, D, T), BF),
            pltpu.VMEM((4, 4, SR, 128), F32),
            pltpu.VMEM((4, 4, SR, 128), BF),
            pltpu.VMEM((4, 4, SR, 128), BF),
            pltpu.VMEM((4, 4, SR, 128), BF),
            pltpu.VMEM((3, 4, SR, 128), BF),
            pltpu.VMEM((4, SR, 128), F32),
            pltpu.VMEM((4, SR, 128), BF),
            pltpu.VMEM((3, SR, 128), BF),
            pltpu.VMEM((2, 4, 4, SR, 128), BF),
            pltpu.VMEM((4 * T, D), BF),
            pltpu.VMEM((NC, 4 * T, CW), BF),
            dma((NC + 3,)),
            dma, dma((NC, 2, 16)),
            dma, dma((3, QP)),
            dma, dma,
            dma((4,)), dma((4,)),
            dma((3,)), dma((3,)),
            dma((3,)), dma((3,)),
            dma((4,)), dma((4,)),
            dma((4,)), dma((4,)),
            dma((NC, 3)), dma((NC, 3)),
            pltpu.SemaphoreType.REGULAR, pltpu.SemaphoreType.REGULAR,
        ],
        compiler_params=pltpu.CompilerParams(
            collective_id=0, has_side_effects=True, vmem_limit_bytes=56 * 1024 * 1024
        ),
        name="attend_project",
    )(view(asked_for), view(offered), view(contents), out_weight)
    return out.reshape(1, T, D)


def solution(mesh):
    in_specs = (
        P("batch", "ctx", None, None),
        P("batch", "ctx", None, None),
        P("batch", "ctx", None, None),
        P("batch", None),
    )
    return jax.shard_map(shards, mesh=mesh, in_specs=in_specs, out_specs=P("batch", "ctx", None), check_vma=False)
```

```python
import jax
import jax.numpy as jnp
from jax import lax
from jax.experimental import pallas as pl
from jax.experimental.pallas import tpu as pltpu
from jax.sharding import PartitionSpec as P

BF = jnp.bfloat16
F32 = jnp.float32
MESH = pl.DeviceIdType.MESH
D = 4096
T = 128
NC = 4
CW = 256
SR = 80
QP = 16


def feature(x):
    return jnp.log(1.0 + jnp.exp(x.astype(F32))).astype(BF)


def pack(s):
    m = s[64:72]
    hi = m.astype(BF).astype(F32)
    return jnp.concatenate([s[0:64], hi, m - hi], axis=0).astype(BF)


def unpack(b):
    f = b.astype(F32)
    m = f[64:72] + f[72:80]
    return jnp.concatenate([f[0:64], m, m], axis=0)


def kernel(
    q_hbm, k_hbm, v_hbm, w_hbm, out_ref,
    wbuf, qbuf, kbuf, vbuf, qf, st, dsend, drecv, r1s, r1r, acc, r2s, r2r, gat, rhs, mixed, obuf,
    lsem, w_ss, w_rs, q_ss, q_rs, d_ss, d_rs, r1_ss, r1_rs, r2_ss, r2_rs, g2_ss, g2_rs, g1_ss, g1_rs,
    gd_ss, gd_rs, o_ss, o_rs, semA, semB,
):
    b = lax.axis_index("batch")
    t = lax.axis_index("ctx")
    y, x = b // 4, b % 4
    z, core = t // 2, t % 2
    zp = z % 2
    me = 2 * zp + core
    sib = 2 * zp + (1 - core)
    zo = z + 1 - 2 * zp
    cls, m0 = z % 4, z // 4

    def dev(dy=0, dx=0, zz=None, cc=None):
        zz = z if zz is None else zz
        cc = core if cc is None else cc
        return (((y + dy) % 4) * 4 + (x + dx) % 4, zz * 2 + cc)

    def zdev(dz):
        return dev(zz=(z + dz + 16) % 16)

    lw = [
        pltpu.make_async_copy(
            w_hbm.at[:, pl.ds(pl.multiple_of(me * (NC * CW) + c * CW, CW), CW)],
            wbuf.at[c, pl.ds(pl.multiple_of(b * 256, 256), 256), :],
            lsem.at[c],
        )
        for c in range(NC)
    ]
    lk = pltpu.make_async_copy(k_hbm, kbuf, lsem.at[NC])
    lv = pltpu.make_async_copy(v_hbm, vbuf, lsem.at[NC + 1])
    lq = pltpu.make_async_copy(q_hbm, qbuf.at[me], lsem.at[NC + 2])
    for c in lw + [lk, lv, lq]:
        c.start()

    barrier = pltpu.get_barrier_semaphore()
    near = [
        dev(dx=1), dev(dx=3), dev(dy=1), dev(dy=3), dev(cc=1 - core),
        zdev(1), zdev(-1), zdev(2), zdev(-2), dev(zz=zo, cc=1 - core),
    ]
    for d in near:
        pl.semaphore_signal(barrier, inc=1, device_id=d, device_id_type=MESH)
    pl.semaphore_wait(barrier, len(near))
    for d in (zdev(2), zdev(-2)):
        pl.semaphore_signal(semA, inc=1, device_id=d, device_id_type=MESH)

    def wcopy(c, h, dy, dx, ty=0, tx=0):
        blk = ((y + dy) % 4) * 4 + (x + dx) % 4
        ref = wbuf.at[c, pl.ds(pl.multiple_of(blk * 256 + h * 128, 128), 128), :]
        return pltpu.make_async_remote_copy(
            src_ref=ref, dst_ref=ref, send_sem=w_ss,
            recv_sem=w_rs.at[c, h, ((dy - ty) % 4) * 4 + (dx - tx) % 4],
            device_id=dev(dy=ty % 4, dx=tx % 4), device_id_type=MESH,
        )

    def wd(h, dp, ds):
        return (ds % 4, dp % 4) if h == 0 else (dp % 4, ds % 4)

    def wsend(c, h, dp, ds, tp, ts):
        wcopy(c, h, *wd(h, dp, ds), *wd(h, tp, ts)).start()

    def wwait(c, h, dp, ds):
        wcopy(c, h, *wd(h, dp, ds)).wait_recv()

    def e0(c):
        for h in (0, 1):
            for tp, ts in ((1, 0), (-1, 0), (0, 1), (0, -1)):
                wsend(c, h, 0, 0, tp, ts)

    def e1(c):
        for h in (0, 1):
            wwait(c, h, -1, 0)
            if c % 2 == 0:
                wsend(c, h, -1, 0, 1, 0)
            wsend(c, h, -1, 0, 0, 1)
            wsend(c, h, -1, 0, 0, -1)
            wwait(c, h, 1, 0)
            if c % 2 == 1:
                wsend(c, h, 1, 0, -1, 0)
            wsend(c, h, 1, 0, 0, 1)
            wsend(c, h, 1, 0, 0, -1)

    def e3(c):
        for h in (0, 1):
            wwait(c, h, 2, 0)
            wsend(c, h, 2, 0, 0, 1)
            wsend(c, h, 2, 0, 0, -1)

    def e4(c):
        for h in (0, 1):
            for dp, ds in ((0, -1), (-1, 1), (1, -1), (2, 1)):
                wwait(c, h, dp, ds)
                wsend(c, h, dp, ds, 0, -ds)

    def e5(c):
        for h in (0, 1):
            for dp, ds in ((0, 1), (1, 1), (-1, -1), (2, -1), (0, 2), (1, 2), (-1, 2), (2, 2)):
                wwait(c, h, dp, ds)

    qr = D // QP

    def qcopy(slot, i, n, target, path):
        ref = qbuf.at[slot, pl.ds(i * qr, n * qr), :]
        return pltpu.make_async_remote_copy(
            src_ref=ref, dst_ref=ref, send_sem=q_ss, recv_sem=q_rs.at[path, i], device_id=target, device_id_type=MESH
        )

    zs = 2 * (1 - zp) + core
    zs2 = 2 * (1 - zp) + (1 - core)

    def qlink(lo, hi):
        for i in range(lo, hi):
            qcopy(me, i, 1, dev(zz=zo), 1).start()

    def qrelay(lo, hi):
        for i in range(lo, hi):
            qcopy(zs, i, 1, dev(zz=zo), 1).wait_recv()
            qcopy(zs, i, 1, dev(cc=1 - core), 2).start()

    def qfeat(slot, lo, hi):
        def body(i, _):
            r = pl.ds(pl.multiple_of(i * 128, 128), 128)
            qf[pl.ds(pl.multiple_of(slot * T, T), T), r] = feature(qbuf[slot, r, :]).T
            return 0
        lax.fori_loop(lo * (32 // QP), hi * (32 // QP), body, 0, unroll=2)

    def start():
        for c in range(NC):
            lw[c].wait()
            e0(c)
        lq.wait()
        qcopy(me, 0, QP, dev(cc=1 - core), 0).start()
        qlink(0, 3)

    lane = lax.broadcasted_iota(jnp.int32, (64, 128), 1) < 64
    nt = (((1,), (1,)), ((), ()))

    def partial(half, i):
        k, m = i // 4, i % 4
        r = pl.ds(pl.multiple_of((16 * half + 4 * m + k) * 128, 128), 128)
        kf = feature(kbuf[r, :])
        g = lax.dot_general(kf, vbuf[r, :], nt, preferred_element_type=F32)
        n = lax.dot_general(jnp.ones((16, 128), BF), kf, nt, preferred_element_type=F32)
        return k, m, jnp.concatenate([jnp.where(lane, g[0:64], g[64:128]), n], axis=0)

    dcopy = pltpu.make_async_remote_copy(
        src_ref=dsend, dst_ref=drecv, send_sem=d_ss, recv_sem=d_rs, device_id=dev(cc=1 - core), device_id_type=MESH
    )

    def theirs():
        lk.wait()
        lv.wait()

        def body(i, _):
            k, m, s = partial(1 - core, i)
            dsend[k, m] = pack(s)
            return 0

        lax.fori_loop(0, 16, body, 0, unroll=4)
        dcopy.start()

    def mine():
        def body(i, _):
            k, m, s = partial(core, i)
            st[k, m] = s
            return 0

        lax.fori_loop(0, 16, body, 0, unroll=4)

    def r1copy(n):
        dz, slot, lo, cnt = ((1, 0, 0, 4), (-1, 1, 0, 4), (2, 2, 0, 2), (-2, 2, 2, 2))[n]
        k = (z + dz + 16) % 4
        return pltpu.make_async_remote_copy(
            src_ref=r1s.at[k, pl.ds(lo, cnt)], dst_ref=r1r.at[slot, pl.ds(lo, cnt)],
            send_sem=r1_ss.at[n], recv_sem=r1_rs.at[n], device_id=zdev(dz), device_id_type=MESH,
        )

    def chip_sum():
        dcopy.wait_recv()

        def body(i, _):
            k, m = i // 4, i % 4
            s = st[k, m] + unpack(drecv[k, m])
            st[k, m] = s
            r1s[k, m] = pack(s)
            return 0

        lax.fori_loop(0, 16, body, 0, unroll=4)
        for n in (2, 3, 0, 1):
            r1copy(n).start()

    def far_ready():
        pl.semaphore_wait(semA, 2)
        for d in (zdev(4), zdev(-4)):
            pl.semaphore_signal(semB, inc=1, device_id=d, device_id_type=MESH)

    def r2copy(r):
        return pltpu.make_async_remote_copy(
            src_ref=r2s.at[(m0 + r) % 4], dst_ref=r2r.at[r - 1],
            send_sem=r2_ss.at[r - 1], recv_sem=r2_rs.at[r - 1], device_id=zdev(4 * r), device_id_type=MESH,
        )

    def near_sum():
        for n in (0, 1, 2, 3):
            r1copy(n).wait_recv()

        def body(m, _):
            s = st[cls, m] + unpack(r1r[0, m]) + unpack(r1r[1, m]) + unpack(r1r[2, m])
            acc[m] = s
            r2s[m] = pack(s)
            return 0

        lax.fori_loop(0, 4, body, 0)
        pl.semaphore_wait(semB, 2)
        for r in (2, 1, 3):
            r2copy(r).start()

    def g2copy(r):
        ref = gat.at[core, cls, m0]
        return pltpu.make_async_remote_copy(
            src_ref=ref, dst_ref=ref, send_sem=g2_ss.at[r - 1], recv_sem=g2_rs.at[r - 1],
            device_id=zdev(4 * r), device_id_type=MESH,
        )

    def far_sum():
        for r in (1, 2, 3):
            r2copy(r).wait_recv()
        total = (acc[m0] + unpack(r2r[0]) + unpack(r2r[1]) + unpack(r2r[2])) * (1.0 / (32 * T))
        gat[core, cls, m0] = pack(total)
        for r in (2, 1, 3):
            g2copy(r).start()

    def g1copy(n):
        dz, lo, cnt = ((1, 0, 4), (-1, 0, 4), (2, 0, 2), (-2, 2, 2))[n]
        ref = gat.at[core, cls, pl.ds(lo, cnt)]
        return pltpu.make_async_remote_copy(
            src_ref=ref, dst_ref=ref, send_sem=g1_ss.at[n], recv_sem=g1_rs.at[n],
            device_id=zdev(dz), device_id_type=MESH,
        )

    def gdcopy(dk):
        ref = gat.at[core, (cls + dk) % 4]
        return pltpu.make_async_remote_copy(
            src_ref=ref, dst_ref=ref, send_sem=gd_ss.at[dk], recv_sem=gd_rs.at[dk],
            device_id=dev(cc=1 - core), device_id_type=MESH,
        )

    def far_back():
        for r in (1, 2, 3):
            g2copy(r).wait_recv()
        for n in (2, 3, 0, 1):
            g1copy(n).start()
        gdcopy(0).start()
        prep(core, cls)

    def take(dk):
        for n in {3: (0,), 1: (1,), 2: (2, 3)}[dk]:
            g1copy(n).wait_recv()
        gdcopy(dk).start()
        prep(core, (cls + dk) % 4)

    def twin(dk):
        gdcopy(dk).wait_recv()
        prep(1 - core, (cls + dk) % 4)

    def prep(half, k):
        row = lax.broadcasted_iota(jnp.int32, (16, 256), 0)
        col = lax.broadcasted_iota(jnp.int32, (16, 256), 1) // 128
        pick = jnp.where(row == 8 * col, 1.0 / 64.0, 0.0).astype(BF)
        zero = jnp.zeros((128, 128), BF)
        for m in range(4):
            s = gat[half, k, m]
            a = s[0:64].astype(F32)
            n = lax.dot_general(s[64:80], pick, (((0,), (0,)), ((), ())), preferred_element_type=F32)
            pair = 16 * half + 4 * m + k
            rhs[pair, 0:64, 0:128] = jnp.where(lane, a, 0.0).astype(BF)
            rhs[pair, 64:128, 0:128] = jnp.where(lane, 0.0, a).astype(BF)
            rhs[pair, 128:256, 0:128] = zero
            rhs[pair, 0:64, 128:256] = jnp.where(lane, n[0:64, 0:128], 0.0).astype(BF)
            rhs[pair, 64:128, 128:256] = jnp.where(lane, 0.0, n[64:128, 0:128]).astype(BF)
            rhs[pair, 128:192, 128:256] = jnp.where(lane, n[0:64, 128:256], 0.0).astype(BF)
            rhs[pair, 192:256, 128:256] = jnp.where(lane, 0.0, n[64:128, 128:256]).astype(BF)

    def mix(lo, hi):
        def body(i, _):
            for j in range(4):
                pair = 4 * i + j
                r = pl.ds(pl.multiple_of(pair * 128, 128), 128)
                w = rhs[pair]
                for u in range(4):
                    f = qf[u * T : (u + 1) * T, r]
                    g = jnp.dot(jnp.concatenate([f, f], axis=1), w, preferred_element_type=F32)
                    mixed[u * T : (u + 1) * T, r] = (g[:, 0:128] / (g[:, 128:256] + 1e-3 / 64.0)).astype(BF)
            return 0

        lax.fori_loop(lo // 4, hi // 4, body, 0)

    def ocopy(c, r):
        s = (me + r) % 4
        return pltpu.make_async_remote_copy(
            src_ref=obuf.at[c, pl.ds(pl.multiple_of(s * T, T), T), :],
            dst_ref=out_ref.at[:, pl.ds(pl.multiple_of(me * (NC * CW) + c * CW, CW), CW)],
            send_sem=o_ss.at[c, r - 1], recv_sem=o_rs.at[c, r - 1],
            device_id=dev(zz=z - zp + s // 2, cc=s % 2), device_id_type=MESH,
        )

    def project(c):
        for i in (0, 1):
            rows = pl.ds(i * 2 * T, 2 * T)
            obuf[c, rows] = jnp.dot(mixed[rows, :], wbuf[c], preferred_element_type=F32).astype(BF)
        for r in (2, 1, 3):
            ocopy(c, r).start()
        out_ref[:, pl.ds(pl.multiple_of(me * (NC * CW) + c * CW, CW), CW)] = obuf[c, pl.ds(pl.multiple_of(me * T, T), T), :]

    def qtwin(lo, hi):
        for i in range(lo, hi):
            qcopy(zs2, i, 1, dev(cc=1 - core), 2).wait_recv()

    def o_wait():
        for c in range(NC):
            for r in (1, 2, 3):
                ocopy(c, r).wait_recv()

    def finish():
        for c in range(NC):
            for r in (1, 2, 3):
                ocopy(c, r).wait_send()
        dcopy.wait_send()
        for n in range(4):
            r1copy(n).wait_send()
            g1copy(n).wait_send()
            gdcopy(n).wait_send()
        for r in (1, 2, 3):
            r2copy(r).wait_send()
            g2copy(r).wait_send()
        wref = wbuf.at[:, pl.ds(0, 3840), :]
        pltpu.make_async_copy(wref, wref, w_ss).wait()
        qref = qbuf.at[pl.ds(0, 3)]
        pltpu.make_async_copy(qref, qref, q_ss).wait()

    plan = [
        ("start", start),
        ("theirs", theirs),
        ("mine", mine),
        ("chip_sum", chip_sum),
        ("qlink1", lambda: qlink(3, 4)),
        ("e1_0", lambda: e1(0)),
        ("far_ready", far_ready),
        ("e1_1", lambda: e1(1)),
        ("near_sum", near_sum),
        ("qlink2", lambda: qlink(4, 8)),
        ("e1_2", lambda: e1(2)),
        ("qf_me", lambda: qfeat(me, 0, QP)),
        ("e1_3", lambda: e1(3)),
        ("qsib", lambda: qcopy(me, 0, QP, dev(cc=1 - core), 0).wait_recv()),
        ("qf_sib", lambda: qfeat(sib, 0, QP)),
        ("e3_0", lambda: e3(0)),
        ("far_sum", far_sum),
        ("qlink3", lambda: qlink(8, 12)),
        ("qrelay1", lambda: qrelay(0, 4)),
        ("e3_1", lambda: e3(1)),
        ("qf_zs", lambda: qfeat(zs, 0, 4)),
        ("qrelay2", lambda: qrelay(4, 8)),
        ("qf_zs2", lambda: qfeat(zs, 4, 8)),
        ("qtwin1", lambda: qtwin(0, 8)),
        ("qf_tw1", lambda: qfeat(zs2, 0, 8)),
        ("e3_2", lambda: e3(2)),
        ("far_back", far_back),
        ("qlink4", lambda: qlink(12, QP)),
        ("e3_3", lambda: e3(3)),
        ("twin0", lambda: twin(0)),
        ("e4_0", lambda: e4(0)),
        ("take3", lambda: take(3)),
        ("take1", lambda: take(1)),
        ("twin3", lambda: twin(3)),
        ("twin1", lambda: twin(1)),
        ("take2", lambda: take(2)),
        ("e4_1", lambda: e4(1)),
        ("twin2", lambda: twin(2)),
        ("mix0", lambda: mix(0, 16)),
        ("e4_2", lambda: e4(2)),
        ("qrelay3", lambda: qrelay(8, QP)),
        ("qf_zs3", lambda: qfeat(zs, 8, QP)),
        ("qtwin2", lambda: qtwin(8, QP)),
        ("qf_tw2", lambda: qfeat(zs2, 8, QP)),
        ("mix1", lambda: mix(16, 32)),
        ("e5_0", lambda: e5(0)),
        ("pr_0", lambda: project(0)),
        ("e4_3", lambda: e4(3)),
        ("e5_1", lambda: e5(1)),
        ("pr_1", lambda: project(1)),
        ("e5_2", lambda: e5(2)),
        ("pr_2", lambda: project(2)),
        ("e5_3", lambda: e5(3)),
        ("pr_3", lambda: project(3)),
        ("o_wait", o_wait),
        ("finish", finish),
    ]
    for name, step in plan:
        step()


def shards(asked_for, offered, contents, out_weight):
    def view(a):
        return jnp.transpose(a, (0, 2, 3, 1)).reshape(D, T)

    dma = pltpu.SemaphoreType.DMA
    hbm = pl.BlockSpec(memory_space=pl.ANY)
    out = pl.pallas_call(
        kernel,
        out_shape=jax.ShapeDtypeStruct((T, D), BF),
        in_specs=[hbm] * 4,
        out_specs=pl.BlockSpec(memory_space=pltpu.VMEM),
        scratch_shapes=[
            pltpu.VMEM((NC, D, CW), BF),
            pltpu.VMEM((4, D, T), BF),
            pltpu.VMEM((D, T), BF),
            pltpu.VMEM((D, T), BF),
            pltpu.VMEM((4 * T, D), BF),
            pltpu.VMEM((4, 4, SR, 128), F32),
            pltpu.VMEM((4, 4, SR, 128), BF),
            pltpu.VMEM((4, 4, SR, 128), BF),
            pltpu.VMEM((4, 4, SR, 128), BF),
            pltpu.VMEM((3, 4, SR, 128), BF),
            pltpu.VMEM((4, SR, 128), F32),
            pltpu.VMEM((4, SR, 128), BF),
            pltpu.VMEM((3, SR, 128), BF),
            pltpu.VMEM((2, 4, 4, SR, 128), BF),
            pltpu.VMEM((32, 256, 256), BF),
            pltpu.VMEM((4 * T, D), BF),
            pltpu.VMEM((NC, 4 * T, CW), BF),
            dma((NC + 3,)),
            dma, dma((NC, 2, 16)),
            dma, dma((3, QP)),
            dma, dma,
            dma((4,)), dma((4,)),
            dma((3,)), dma((3,)),
            dma((3,)), dma((3,)),
            dma((4,)), dma((4,)),
            dma((4,)), dma((4,)),
            dma((NC, 3)), dma((NC, 3)),
            pltpu.SemaphoreType.REGULAR, pltpu.SemaphoreType.REGULAR,
        ],
        compiler_params=pltpu.CompilerParams(
            collective_id=0, has_side_effects=True, vmem_limit_bytes=56 * 1024 * 1024
        ),
        name="attend_project",
    )(view(asked_for), view(offered), view(contents), out_weight)
    return out.reshape(1, T, D)


def solution(mesh):
    in_specs = (
        P("batch", "ctx", None, None),
        P("batch", "ctx", None, None),
        P("batch", "ctx", None, None),
        P("batch", None),
    )
    return jax.shard_map(shards, mesh=mesh, in_specs=in_specs, out_specs=P("batch", "ctx", None), check_vma=False)
```

```python
import jax
import jax.numpy as jnp
from jax import lax
from jax.experimental import pallas as pl
from jax.experimental.pallas import tpu as pltpu
from jax.sharding import PartitionSpec as P

BF = jnp.bfloat16
F32 = jnp.float32
MESH = pl.DeviceIdType.MESH
D = 4096
T = 128
NC = 4
CW = 256
SR = 80
QP = 16


def feature(x):
    return jnp.log(1.0 + jnp.exp(x.astype(F32))).astype(BF)


def pack(s):
    m = s[64:72]
    hi = m.astype(BF).astype(F32)
    return jnp.concatenate([s[0:64], hi, m - hi], axis=0).astype(BF)


def unpack(b):
    f = b.astype(F32)
    m = f[64:72] + f[72:80]
    return jnp.concatenate([f[0:64], m, m], axis=0)


def kernel(
    q_hbm, k_hbm, v_hbm, w_hbm, out_ref,
    wbuf, qbuf, kbuf, vbuf, qf, st, dsend, drecv, r1s, r1r, acc, r2s, r2r, gat, rhs, mixed, obuf,
    lsem, w_ss, w_rs, q_ss, q_rs, d_ss, d_rs, r1_ss, r1_rs, r2_ss, r2_rs, g2_ss, g2_rs, g1_ss, g1_rs,
    gd_ss, gd_rs, o_ss, o_rs, semA, semB,
):
    b = lax.axis_index("batch")
    t = lax.axis_index("ctx")
    y, x = b // 4, b % 4
    z, core = t // 2, t % 2
    zp = z % 2
    quarter = 2 * zp + core
    me, sib, zs, zs2 = core, 1 - core, 2 + core, 3 - core
    znext = (z + 2 * core + 15) % 16
    zback = (z - 2 * core + 17) % 16
    cls, m0 = z % 4, z // 4

    def dev(dy=0, dx=0, zz=None, cc=None):
        zz = z if zz is None else zz
        cc = core if cc is None else cc
        return (((y + dy) % 4) * 4 + (x + dx) % 4, zz * 2 + cc)

    def zdev(dz):
        return dev(zz=(z + dz + 16) % 16)

    lw = [
        pltpu.make_async_copy(
            w_hbm.at[:, pl.ds(pl.multiple_of(quarter * (NC * CW) + c * CW, CW), CW)],
            wbuf.at[c, pl.ds(pl.multiple_of(b * 256, 256), 256), :],
            lsem.at[c],
        )
        for c in range(NC)
    ]
    lk = pltpu.make_async_copy(k_hbm, kbuf, lsem.at[NC])
    lv = pltpu.make_async_copy(v_hbm, vbuf, lsem.at[NC + 1])
    lq = pltpu.make_async_copy(q_hbm, qbuf.at[me], lsem.at[NC + 2])
    for c in lw + [lk, lv, lq]:
        c.start()

    barrier = pltpu.get_barrier_semaphore()
    near = [
        dev(dx=1), dev(dx=3), dev(dy=1), dev(dy=3), dev(cc=1 - core),
        zdev(1), zdev(-1), zdev(2), zdev(-2), dev(zz=znext, cc=1 - core),
    ]
    for d in near:
        pl.semaphore_signal(barrier, inc=1, device_id=d, device_id_type=MESH)
    pl.semaphore_wait(barrier, len(near))
    for d in (zdev(2), zdev(-2)):
        pl.semaphore_signal(semA, inc=1, device_id=d, device_id_type=MESH)

    def wcopy(c, h, dy, dx, ty=0, tx=0):
        blk = ((y + dy) % 4) * 4 + (x + dx) % 4
        ref = wbuf.at[c, pl.ds(pl.multiple_of(blk * 256 + h * 128, 128), 128), :]
        return pltpu.make_async_remote_copy(
            src_ref=ref, dst_ref=ref, send_sem=w_ss,
            recv_sem=w_rs.at[c, h, ((dy - ty) % 4) * 4 + (dx - tx) % 4],
            device_id=dev(dy=ty % 4, dx=tx % 4), device_id_type=MESH,
        )

    def wd(h, dp, ds):
        return (ds % 4, dp % 4) if h == 0 else (dp % 4, ds % 4)

    def wsend(c, h, dp, ds, tp, ts):
        wcopy(c, h, *wd(h, dp, ds), *wd(h, tp, ts)).start()

    def wwait(c, h, dp, ds):
        wcopy(c, h, *wd(h, dp, ds)).wait_recv()

    def e0(c):
        for h in (0, 1):
            for tp, ts in ((1, 0), (-1, 0), (0, 1), (0, -1)):
                wsend(c, h, 0, 0, tp, ts)

    def e1(c):
        for h in (0, 1):
            wwait(c, h, -1, 0)
            if c % 2 == 0:
                wsend(c, h, -1, 0, 1, 0)
            wsend(c, h, -1, 0, 0, 1)
            wsend(c, h, -1, 0, 0, -1)
            wwait(c, h, 1, 0)
            if c % 2 == 1:
                wsend(c, h, 1, 0, -1, 0)
            wsend(c, h, 1, 0, 0, 1)
            wsend(c, h, 1, 0, 0, -1)

    def e3(c):
        for h in (0, 1):
            wwait(c, h, 2, 0)
            wsend(c, h, 2, 0, 0, 1)
            wsend(c, h, 2, 0, 0, -1)

    def e4(c):
        for h in (0, 1):
            for dp, ds in ((0, -1), (-1, 1), (1, -1), (2, 1)):
                wwait(c, h, dp, ds)
                wsend(c, h, dp, ds, 0, -ds)

    def e5(c):
        for h in (0, 1):
            for dp, ds in ((0, 1), (1, 1), (-1, -1), (2, -1), (0, 2), (1, 2), (-1, 2), (2, 2)):
                wwait(c, h, dp, ds)

    qr = D // QP

    def qcopy(slot, to, i, n, target, path):
        r = pl.ds(i * qr, n * qr)
        return pltpu.make_async_remote_copy(
            src_ref=qbuf.at[slot, r, :], dst_ref=qbuf.at[to, r, :], send_sem=q_ss, recv_sem=q_rs.at[path, i],
            device_id=target, device_id_type=MESH,
        )

    def qlink(lo, hi):
        for i in range(lo, hi):
            qcopy(me, zs, i, 1, dev(zz=znext), 1).start()

    def qrelay(lo, hi):
        for i in range(lo, hi):
            qcopy(zs, zs, i, 1, dev(cc=1 - core), 1).wait_recv()
            qcopy(zs, zs, i, 1, dev(cc=1 - core), 2).start()

    def qfeat(slot, lo, hi):
        def body(i, _):
            r = pl.ds(pl.multiple_of(i * 128, 128), 128)
            qf[pl.ds(pl.multiple_of(slot * T, T), T), r] = feature(qbuf[slot, r, :]).T
            return 0
        lax.fori_loop(lo * (32 // QP), hi * (32 // QP), body, 0, unroll=2)

    def start():
        for c in range(NC):
            lw[c].wait()
            e0(c)
        lq.wait()
        qcopy(me, me, 0, QP, dev(cc=1 - core), 0).start()
        qlink(0, 4)

    lane = lax.broadcasted_iota(jnp.int32, (64, 128), 1) < 64
    nt = (((1,), (1,)), ((), ()))

    def partial(half, i):
        k, m = i // 4, i % 4
        r = pl.ds(pl.multiple_of((16 * half + 4 * m + k) * 128, 128), 128)
        kf = feature(kbuf[r, :])
        g = lax.dot_general(kf, vbuf[r, :], nt, preferred_element_type=F32)
        n = lax.dot_general(jnp.ones((16, 128), BF), kf, nt, preferred_element_type=F32)
        return k, m, jnp.concatenate([jnp.where(lane, g[0:64], g[64:128]), n], axis=0)

    dcopy = pltpu.make_async_remote_copy(
        src_ref=dsend, dst_ref=drecv, send_sem=d_ss, recv_sem=d_rs, device_id=dev(cc=1 - core), device_id_type=MESH
    )

    def theirs():
        lk.wait()
        lv.wait()

        def body(i, _):
            k, m, s = partial(1 - core, i)
            dsend[k, m] = pack(s)
            return 0

        lax.fori_loop(0, 16, body, 0, unroll=4)
        dcopy.start()

    def mine():
        def body(i, _):
            k, m, s = partial(core, i)
            st[k, m] = s
            return 0

        lax.fori_loop(0, 16, body, 0, unroll=4)

    def r1copy(n):
        dz, slot, lo, cnt = ((1, 0, 0, 4), (-1, 1, 0, 4), (2, 2, 0, 2), (-2, 2, 2, 2))[n]
        k = (z + dz + 16) % 4
        return pltpu.make_async_remote_copy(
            src_ref=r1s.at[k, pl.ds(lo, cnt)], dst_ref=r1r.at[slot, pl.ds(lo, cnt)],
            send_sem=r1_ss.at[n], recv_sem=r1_rs.at[n], device_id=zdev(dz), device_id_type=MESH,
        )

    def chip_sum():
        dcopy.wait_recv()

        def body(i, _):
            k, m = i // 4, i % 4
            s = st[k, m] + unpack(drecv[k, m])
            st[k, m] = s
            r1s[k, m] = pack(s)
            return 0

        lax.fori_loop(0, 16, body, 0, unroll=4)
        for n in (2, 3, 0, 1):
            r1copy(n).start()

    def far_ready():
        pl.semaphore_wait(semA, 2)
        for d in (zdev(4), zdev(-4)):
            pl.semaphore_signal(semB, inc=1, device_id=d, device_id_type=MESH)

    def r2copy(r):
        return pltpu.make_async_remote_copy(
            src_ref=r2s.at[(m0 + r) % 4], dst_ref=r2r.at[r - 1],
            send_sem=r2_ss.at[r - 1], recv_sem=r2_rs.at[r - 1], device_id=zdev(4 * r), device_id_type=MESH,
        )

    def near_sum():
        for n in (0, 1, 2, 3):
            r1copy(n).wait_recv()

        def body(m, _):
            s = st[cls, m] + unpack(r1r[0, m]) + unpack(r1r[1, m]) + unpack(r1r[2, m])
            acc[m] = s
            r2s[m] = pack(s)
            return 0

        lax.fori_loop(0, 4, body, 0)
        pl.semaphore_wait(semB, 2)
        for r in (2, 1, 3):
            r2copy(r).start()

    def g2copy(r):
        ref = gat.at[core, cls, m0]
        return pltpu.make_async_remote_copy(
            src_ref=ref, dst_ref=ref, send_sem=g2_ss.at[r - 1], recv_sem=g2_rs.at[r - 1],
            device_id=zdev(4 * r), device_id_type=MESH,
        )

    def far_sum():
        for r in (1, 2, 3):
            r2copy(r).wait_recv()
        total = (acc[m0] + unpack(r2r[0]) + unpack(r2r[1]) + unpack(r2r[2])) * (1.0 / (32 * T))
        gat[core, cls, m0] = pack(total)
        for r in (2, 1, 3):
            g2copy(r).start()

    def g1copy(n):
        dz, lo, cnt = ((1, 0, 4), (-1, 0, 4), (2, 0, 2), (-2, 2, 2))[n]
        ref = gat.at[core, cls, pl.ds(lo, cnt)]
        return pltpu.make_async_remote_copy(
            src_ref=ref, dst_ref=ref, send_sem=g1_ss.at[n], recv_sem=g1_rs.at[n],
            device_id=zdev(dz), device_id_type=MESH,
        )

    def gdcopy(dk):
        ref = gat.at[core, (cls + dk) % 4]
        return pltpu.make_async_remote_copy(
            src_ref=ref, dst_ref=ref, send_sem=gd_ss.at[dk], recv_sem=gd_rs.at[dk],
            device_id=dev(cc=1 - core), device_id_type=MESH,
        )

    def far_back():
        for r in (1, 2, 3):
            g2copy(r).wait_recv()
        for n in (2, 3, 0, 1):
            g1copy(n).start()
        gdcopy(0).start()
        prep(core, cls)

    def take(dk):
        for n in {3: (0,), 1: (1,), 2: (2, 3)}[dk]:
            g1copy(n).wait_recv()
        gdcopy(dk).start()
        prep(core, (cls + dk) % 4)

    def twin(dk):
        gdcopy(dk).wait_recv()
        prep(1 - core, (cls + dk) % 4)

    def prep(half, k):
        row = lax.broadcasted_iota(jnp.int32, (16, 256), 0)
        col = lax.broadcasted_iota(jnp.int32, (16, 256), 1) // 128
        pick = jnp.where(row == 8 * col, 1.0 / 64.0, 0.0).astype(BF)
        zero = jnp.zeros((128, 128), BF)
        for m in range(4):
            s = gat[half, k, m]
            a = s[0:64].astype(F32)
            n = lax.dot_general(s[64:80], pick, (((0,), (0,)), ((), ())), preferred_element_type=F32)
            pair = 16 * half + 4 * m + k
            rhs[pair, 0:64, 0:128] = jnp.where(lane, a, 0.0).astype(BF)
            rhs[pair, 64:128, 0:128] = jnp.where(lane, 0.0, a).astype(BF)
            rhs[pair, 128:256, 0:128] = zero
            rhs[pair, 0:64, 128:256] = jnp.where(lane, n[0:64, 0:128], 0.0).astype(BF)
            rhs[pair, 64:128, 128:256] = jnp.where(lane, 0.0, n[64:128, 0:128]).astype(BF)
            rhs[pair, 128:192, 128:256] = jnp.where(lane, n[0:64, 128:256], 0.0).astype(BF)
            rhs[pair, 192:256, 128:256] = jnp.where(lane, 0.0, n[64:128, 128:256]).astype(BF)

    def mix(lo, hi):
        def body(i, _):
            for j in range(4):
                pair = 4 * i + j
                r = pl.ds(pl.multiple_of(pair * 128, 128), 128)
                w = rhs[pair]
                for u in range(4):
                    t0 = pl.ds(u * T, T)
                    f = qf[t0, r]
                    g = jnp.dot(jnp.concatenate([f, f], axis=1), w, preferred_element_type=F32)
                    mixed[t0, r] = (g[:, 0:128] / (g[:, 128:256] + 1e-3 / 64.0)).astype(BF)
            return 0

        lax.fori_loop(lo // 4, hi // 4, body, 0)

    others = ((sib, dev(cc=1 - core)), (zs, dev(zz=zback)), (zs2, dev(zz=znext, cc=1 - core)))

    def rows(slot):
        return pl.ds(pl.multiple_of(slot * T, T), T)

    def cols(c):
        return pl.ds(pl.multiple_of(quarter * (NC * CW) + c * CW, CW), CW)

    def ocopy(c, n):
        s, target = others[n]
        return pltpu.make_async_remote_copy(
            src_ref=obuf.at[c, rows(s), :], dst_ref=out_ref.at[:, cols(c)],
            send_sem=o_ss.at[c, n], recv_sem=o_rs.at[c, n],
            device_id=target, device_id_type=MESH,
        )

    def part(c, slot):
        return jnp.dot(mixed[rows(slot), :], wbuf[c], preferred_element_type=F32).astype(BF)

    def far_tokens(c):
        obuf[c, rows(zs)] = part(c, zs)
        obuf[c, rows(zs2)] = part(c, zs2)
        ocopy(c, 1).start()
        ocopy(c, 2).start()

    def all_tokens(c):
        far = pl.ds(2 * T, 2 * T)
        obuf[c, far] = jnp.dot(mixed[far, :], wbuf[c], preferred_element_type=F32).astype(BF)
        near = pl.ds(0, 2 * T)
        obuf[c, near] = jnp.dot(mixed[near, :], wbuf[c], preferred_element_type=F32).astype(BF)
        for n in (1, 2, 0):
            ocopy(c, n).start()
        out_ref[:, cols(c)] = obuf[c, rows(me)]

    def near_tokens(c):
        obuf[c, rows(sib)] = part(c, sib)
        out_ref[:, cols(c)] = part(c, me)
        ocopy(c, 0).start()

    def qtwin(lo, hi):
        for i in range(lo, hi):
            qcopy(zs2, zs2, i, 1, dev(cc=1 - core), 2).wait_recv()

    def o_wait():
        for c in range(NC):
            for n in (0, 1, 2):
                ocopy(c, n).wait_recv()

    def finish():
        for c in range(NC):
            for n in (0, 1, 2):
                ocopy(c, n).wait_send()
        dcopy.wait_send()
        for n in range(4):
            r1copy(n).wait_send()
            g1copy(n).wait_send()
            gdcopy(n).wait_send()
        for r in (1, 2, 3):
            r2copy(r).wait_send()
            g2copy(r).wait_send()
        wref = wbuf.at[:, pl.ds(0, 3840), :]
        pltpu.make_async_copy(wref, wref, w_ss).wait()
        qref = qbuf.at[pl.ds(0, 3)]
        pltpu.make_async_copy(qref, qref, q_ss).wait()

    plan = [
        ("start", start),
        ("theirs", theirs),
        ("mine", mine),
        ("chip_sum", chip_sum),
        ("qlink1", lambda: qlink(4, 6)),
        ("e1_0", lambda: e1(0)),
        ("far_ready", far_ready),
        ("near_sum", near_sum),
        ("qlink2", lambda: qlink(6, 12)),
        ("e1_1", lambda: e1(1)),
        ("e1_2", lambda: e1(2)),
        ("qf_me", lambda: qfeat(me, 0, QP)),
        ("e1_3", lambda: e1(3)),
        ("qsib", lambda: qcopy(sib, sib, 0, QP, dev(cc=1 - core), 0).wait_recv()),
        ("qf_sib", lambda: qfeat(sib, 0, QP)),
        ("far_sum", far_sum),
        ("qlink3", lambda: qlink(12, QP)),
        ("e3_0", lambda: e3(0)),
        ("qrelay1", lambda: qrelay(0, 8)),
        ("qf_zs", lambda: qfeat(zs, 0, 8)),
        ("e3_1", lambda: e3(1)),
        ("qtwin1", lambda: qtwin(0, 8)),
        ("qf_tw", lambda: qfeat(zs2, 0, 8)),
        ("far_back", far_back),
        ("qrelay2", lambda: qrelay(8, QP)),
        ("qf_zs2", lambda: qfeat(zs, 8, QP)),
        ("e3_2", lambda: e3(2)),
        ("twin0", lambda: twin(0)),
        ("qtwin2", lambda: qtwin(8, QP)),
        ("qf_tw2", lambda: qfeat(zs2, 8, QP)),
        ("e3_3", lambda: e3(3)),
        ("take3", lambda: take(3)),
        ("take1", lambda: take(1)),
        ("e4_0", lambda: e4(0)),
        ("twin3", lambda: twin(3)),
        ("twin1", lambda: twin(1)),
        ("take2", lambda: take(2)),
        ("e4_1", lambda: e4(1)),
        ("twin2", lambda: twin(2)),
        ("mix0", lambda: mix(0, 16)),
        ("e4_2", lambda: e4(2)),
        ("mix1", lambda: mix(16, 32)),
        ("e5_0", lambda: e5(0)),
        ("e4_3", lambda: e4(3)),
        ("pr_0", lambda: all_tokens(0)),
        ("e5_1", lambda: e5(1)),
        ("pr_1", lambda: all_tokens(1)),
        ("e5_2", lambda: e5(2)),
        ("pr_2", lambda: all_tokens(2)),
        ("e5_3", lambda: e5(3)),
        ("prf_3", lambda: far_tokens(3)),
        ("prn_3", lambda: near_tokens(3)),
        ("o_wait", o_wait),
        ("finish", finish),
    ]
    for name, step in plan:
        step()


def shards(asked_for, offered, contents, out_weight):
    def view(a):
        return jnp.transpose(a, (0, 2, 3, 1)).reshape(D, T)

    dma = pltpu.SemaphoreType.DMA
    hbm = pl.BlockSpec(memory_space=pl.ANY)
    out = pl.pallas_call(
        kernel,
        out_shape=pltpu.VMEM((T, D), BF),
        in_specs=[hbm] * 4,
        out_specs=pl.BlockSpec(memory_space=pltpu.VMEM),
        scratch_shapes=[
            pltpu.VMEM((NC, D, CW), BF),
            pltpu.VMEM((4, D, T), BF),
            pltpu.VMEM((D, T), BF),
            pltpu.VMEM((D, T), BF),
            pltpu.VMEM((4 * T, D), BF),
            pltpu.VMEM((4, 4, SR, 128), F32),
            pltpu.VMEM((4, 4, SR, 128), BF),
            pltpu.VMEM((4, 4, SR, 128), BF),
            pltpu.VMEM((4, 4, SR, 128), BF),
            pltpu.VMEM((3, 4, SR, 128), BF),
            pltpu.VMEM((4, SR, 128), F32),
            pltpu.VMEM((4, SR, 128), BF),
            pltpu.VMEM((3, SR, 128), BF),
            pltpu.VMEM((2, 4, 4, SR, 128), BF),
            pltpu.VMEM((32, 256, 256), BF),
            pltpu.VMEM((4 * T, D), BF),
            pltpu.VMEM((NC, 4 * T, CW), BF),
            dma((NC + 3,)),
            dma, dma((NC, 2, 16)),
            dma, dma((3, QP)),
            dma, dma,
            dma((4,)), dma((4,)),
            dma((3,)), dma((3,)),
            dma((3,)), dma((3,)),
            dma((4,)), dma((4,)),
            dma((4,)), dma((4,)),
            dma((NC, 3)), dma((NC, 3)),
            pltpu.SemaphoreType.REGULAR, pltpu.SemaphoreType.REGULAR,
        ],
        compiler_params=pltpu.CompilerParams(
            collective_id=0, has_side_effects=True, vmem_limit_bytes=56 * 1024 * 1024
        ),
        name="attend_project",
    )(view(asked_for), view(offered), view(contents), out_weight)
    return out.reshape(1, T, D)


def solution(mesh):
    in_specs = (
        P("batch", "ctx", None, None),
        P("batch", "ctx", None, None),
        P("batch", "ctx", None, None),
        P("batch", None),
    )
    return jax.shard_map(shards, mesh=mesh, in_specs=in_specs, out_specs=P("batch", "ctx", None), check_vma=False)
```

```python
import jax
import jax.numpy as jnp
from jax import lax
from jax.experimental import pallas as pl
from jax.experimental.pallas import tpu as pltpu
from jax.sharding import PartitionSpec as P

BF = jnp.bfloat16
F32 = jnp.float32
MESH = pl.DeviceIdType.MESH
D = 4096
T = 128
NC = 4
CW = 256
SR = 80
QP = 16


def feature(x):
    return jnp.log(1.0 + jnp.exp(x.astype(F32))).astype(BF)


def pack(s):
    m = s[64:72]
    hi = m.astype(BF).astype(F32)
    return jnp.concatenate([s[0:64], hi, m - hi], axis=0).astype(BF)


def unpack(b):
    f = b.astype(F32)
    m = f[64:72] + f[72:80]
    return jnp.concatenate([f[0:64], m, m], axis=0)


def kernel(
    q_hbm, k_hbm, v_hbm, w_hbm, out_ref,
    wbuf, qbuf, kbuf, vbuf, qf, st, dsend, drecv, r1s, r1r, acc, r2s, r2r, gat, rhs, mixed, obuf,
    lsem, w_ss, w_rs, q_ss, q_rs, s_ss, d_rs, r1_rs, r2_rs, g2_rs, g1_rs, gd_rs, o_ss, o_rs, semA, semB, semP, semZ,
):
    b = lax.axis_index("batch")
    t = lax.axis_index("ctx")
    y, x = b // 4, b % 4
    z, core = t // 2, t % 2
    zp = z % 2
    quarter = 2 * zp + core
    me, sib, zs, zs2 = core, 1 - core, 2 + core, 3 - core
    znext = (z + 2 * core + 15) % 16
    zback = (z - 2 * core + 17) % 16
    cls, m0 = z % 4, z // 4

    def dev(dy=0, dx=0, zz=None, cc=None):
        zz = z if zz is None else zz
        cc = core if cc is None else cc
        return (((y + dy) % 4) * 4 + (x + dx) % 4, zz * 2 + cc)

    def zdev(dz):
        return dev(zz=(z + dz + 16) % 16)

    lw = [
        pltpu.make_async_copy(
            w_hbm.at[:, pl.ds(pl.multiple_of(quarter * (NC * CW) + c * CW, CW), CW)],
            wbuf.at[c, pl.ds(pl.multiple_of(b * 256, 256), 256), :],
            lsem.at[c],
        )
        for c in range(NC)
    ]
    lk = pltpu.make_async_copy(k_hbm, kbuf, lsem.at[NC])
    lv = pltpu.make_async_copy(v_hbm, vbuf, lsem.at[NC + 1])
    lq = pltpu.make_async_copy(q_hbm, qbuf.at[me], lsem.at[NC + 2])
    for c in lw + [lk, lv, lq]:
        c.start()

    barrier = pltpu.get_barrier_semaphore()

    def tell(sem, d):
        pl.semaphore_signal(sem, inc=1, device_id=d, device_id_type=MESH)

    twin_core = dev(cc=1 - core)
    for dy, dx in ((0, 1), (0, 3), (1, 0), (3, 0)):
        tell(barrier, dev(dy=dy, dx=dx, cc=0))
    for dz in (1, -1, 2, -2):
        tell(barrier, dev(zz=(z + dz + 16) % 16, cc=1))

    @pl.when(core == 1)
    def _():
        tell(barrier, twin_core)

    @pl.when(core == 0)
    def _():
        pl.semaphore_wait(barrier, 9)
        tell(semP, twin_core)

    @pl.when(core == 1)
    def _():
        pl.semaphore_wait(semP, 1)

    def z_ready():
        @pl.when(core == 1)
        def _():
            pl.semaphore_wait(barrier, 8)
            tell(semZ, twin_core)

        @pl.when(core == 0)
        def _():
            pl.semaphore_wait(semZ, 1)

        for d in (zdev(2), zdev(-2)):
            tell(semA, d)

    def drain(ref, sem):
        pltpu.make_async_copy(ref, ref, sem).wait()

    groups = {(1, 0): 0, (3, 0): 0, (2, 0): 1, (0, 3): 2, (3, 1): 2, (1, 3): 3, (2, 1): 3}

    def wsend(c, h, dp, ds, tp, ts):
        dy, dx = (ds, dp) if h == 0 else (dp, ds)
        ty, tx = (ts, tp) if h == 0 else (tp, ts)
        blk = ((y + dy + 4) % 4) * 4 + (x + dx + 4) % 4
        ref = wbuf.at[c, pl.ds(pl.multiple_of(blk * 256 + h * 128, 128), 128), :]
        pltpu.make_async_remote_copy(
            src_ref=ref, dst_ref=ref, send_sem=w_ss,
            recv_sem=w_rs.at[c, groups.get(((dp - tp) % 4, (ds - ts) % 4), 4)],
            device_id=dev(dy=ty % 4, dx=tx % 4), device_id_type=MESH,
        ).start()

    def wwait(c, g):
        drain(wbuf.at[c, pl.ds(0, (4, 2, 4, 4, 16)[g] * 128), :], w_rs.at[c, g])

    def e0(c):
        for h in (0, 1):
            for tp, ts in ((1, 0), (-1, 0), (0, 1), (0, -1)):
                wsend(c, h, 0, 0, tp, ts)

    def e1(c):
        wwait(c, 0)
        for h in (0, 1):
            wsend(c, h, *(((-1, 0, 1, 0), (1, 0, -1, 0))[c % 2]))
            for dp in (-1, 1):
                wsend(c, h, dp, 0, 0, 1)
                wsend(c, h, dp, 0, 0, -1)

    def e3(c):
        wwait(c, 1)
        for h in (0, 1):
            wsend(c, h, 2, 0, 0, 1)
            wsend(c, h, 2, 0, 0, -1)

    def e4(c, late):
        wwait(c, 2 + late)
        for h in (0, 1):
            for dp, ds in (((0, -1), (-1, 1)), ((1, -1), (2, 1)))[late]:
                wsend(c, h, dp, ds, 0, -ds)

    def e5(c):
        wwait(c, 4)

    qr = D // QP

    def qcopy(slot, to, i, n, target, sem):
        r = pl.ds(i * qr, n * qr)
        pltpu.make_async_remote_copy(
            src_ref=qbuf.at[slot, r, :], dst_ref=qbuf.at[to, r, :], send_sem=q_ss, recv_sem=q_rs.at[sem],
            device_id=target, device_id_type=MESH,
        ).start()

    def qwait(sem, n):
        drain(qbuf.at[0, pl.ds(0, n * qr), :], q_rs.at[sem])

    def qlink(lo, hi):
        for i in range(lo, hi):
            qcopy(me, zs, i, 1, dev(zz=znext), 1 + i // 8)

    def qrelay(half):
        qwait(1 + half, 8)
        qcopy(zs, zs, 8 * half, 8, twin_core, 3 + half)

    def qfeat(slot, lo, hi):
        def body(i, _):
            r = pl.ds(pl.multiple_of(i * 128, 128), 128)
            qf[pl.ds(pl.multiple_of(slot * T, T), T), r] = feature(qbuf[slot, r, :]).T
            return 0
        lax.fori_loop(lo * (32 // QP), hi * (32 // QP), body, 0, unroll=2)

    def start():
        for c in range(NC):
            lw[c].wait()
            e0(c)
        lq.wait()
        qcopy(me, me, 0, QP, twin_core, 0)

    lane = lax.broadcasted_iota(jnp.int32, (64, 128), 1) < 64
    nt = (((1,), (1,)), ((), ()))

    def partial(half, i):
        k, m = i // 4, i % 4
        r = pl.ds(pl.multiple_of((16 * half + 4 * m + k) * 128, 128), 128)
        kf = feature(kbuf[r, :])
        g = lax.dot_general(kf, vbuf[r, :], nt, preferred_element_type=F32)
        n = lax.dot_general(jnp.ones((16, 128), BF), kf, nt, preferred_element_type=F32)
        return k, m, jnp.concatenate([jnp.where(lane, g[0:64], g[64:128]), n], axis=0)

    dcopy = pltpu.make_async_remote_copy(
        src_ref=dsend, dst_ref=drecv, send_sem=s_ss, recv_sem=d_rs, device_id=dev(cc=1 - core), device_id_type=MESH
    )

    def theirs():
        lk.wait()
        lv.wait()

        def body(i, _):
            k, m, s = partial(1 - core, i)
            dsend[k, m] = pack(s)
            return 0

        lax.fori_loop(0, 16, body, 0, unroll=4)
        dcopy.start()

    def mine():
        def body(i, _):
            k, m, s = partial(core, i)
            st[k, m] = s
            return 0

        lax.fori_loop(0, 16, body, 0, unroll=4)

    def r1copy(n):
        dz, slot, lo, cnt = ((1, 0, 0, 4), (-1, 1, 0, 4), (2, 2, 0, 2), (-2, 2, 2, 2))[n]
        k = (z + dz + 16) % 4
        return pltpu.make_async_remote_copy(
            src_ref=r1s.at[k, pl.ds(lo, cnt)], dst_ref=r1r.at[slot, pl.ds(lo, cnt)],
            send_sem=s_ss, recv_sem=r1_rs, device_id=zdev(dz), device_id_type=MESH,
        )

    def chip_sum():
        dcopy.wait_recv()

        def body(i, _):
            k, m = i // 4, i % 4
            s = st[k, m] + unpack(drecv[k, m])
            st[k, m] = s
            r1s[k, m] = pack(s)
            return 0

        lax.fori_loop(0, 16, body, 0, unroll=4)
        for n in (2, 3, 0, 1):
            r1copy(n).start()

    def far_ready():
        pl.semaphore_wait(semA, 2)
        for d in (zdev(4), zdev(-4)):
            pl.semaphore_signal(semB, inc=1, device_id=d, device_id_type=MESH)

    def r2copy(r):
        return pltpu.make_async_remote_copy(
            src_ref=r2s.at[(m0 + r) % 4], dst_ref=r2r.at[r - 1],
            send_sem=s_ss, recv_sem=r2_rs, device_id=zdev(4 * r), device_id_type=MESH,
        )

    def near_sum():
        drain(r1r, r1_rs)

        def body(m, _):
            s = st[cls, m] + unpack(r1r[0, m]) + unpack(r1r[1, m]) + unpack(r1r[2, m])
            acc[m] = s
            r2s[m] = pack(s)
            return 0

        lax.fori_loop(0, 4, body, 0)
        pl.semaphore_wait(semB, 2)
        for r in (2, 1, 3):
            r2copy(r).start()

    def g2copy(r):
        ref = gat.at[core, cls, m0]
        return pltpu.make_async_remote_copy(
            src_ref=ref, dst_ref=ref, send_sem=s_ss, recv_sem=g2_rs,
            device_id=zdev(4 * r), device_id_type=MESH,
        )

    def far_sum():
        drain(r2r, r2_rs)
        total = (acc[m0] + unpack(r2r[0]) + unpack(r2r[1]) + unpack(r2r[2])) * (1.0 / (32 * T))
        gat[core, cls, m0] = pack(total)
        for r in (2, 1, 3):
            g2copy(r).start()

    def g1copy(n):
        dz, lo, cnt = ((1, 0, 4), (-1, 0, 4), (2, 0, 2), (-2, 2, 2))[n]
        ref = gat.at[core, cls, pl.ds(lo, cnt)]
        return pltpu.make_async_remote_copy(
            src_ref=ref, dst_ref=ref, send_sem=s_ss, recv_sem=g1_rs.at[min(n, 2)],
            device_id=zdev(dz), device_id_type=MESH,
        )

    def gdcopy(dk):
        ref = gat.at[core, (cls + dk) % 4]
        return pltpu.make_async_remote_copy(
            src_ref=ref, dst_ref=ref, send_sem=s_ss, recv_sem=gd_rs.at[dk],
            device_id=dev(cc=1 - core), device_id_type=MESH,
        )

    def far_back():
        drain(r2r, g2_rs)
        for n in (2, 3, 0, 1):
            g1copy(n).start()
        gdcopy(0).start()
        prep(core, cls)

    def take(dk):
        drain(gat.at[core, cls], g1_rs.at[{3: 0, 1: 1, 2: 2}[dk]])
        gdcopy(dk).start()
        prep(core, (cls + dk) % 4)

    def twin(dk):
        gdcopy(dk).wait_recv()
        prep(1 - core, (cls + dk) % 4)

    def prep(half, k):
        row = lax.broadcasted_iota(jnp.int32, (16, 256), 0)
        col = lax.broadcasted_iota(jnp.int32, (16, 256), 1) // 128
        pick = jnp.where(row == 8 * col, 1.0 / 64.0, 0.0).astype(BF)
        zero = jnp.zeros((128, 128), BF)
        for m in range(4):
            s = gat[half, k, m]
            a = s[0:64].astype(F32)
            n = lax.dot_general(s[64:80], pick, (((0,), (0,)), ((), ())), preferred_element_type=F32)
            pair = 16 * half + 4 * m + k
            rhs[pair, 0:64, 0:128] = jnp.where(lane, a, 0.0).astype(BF)
            rhs[pair, 64:128, 0:128] = jnp.where(lane, 0.0, a).astype(BF)
            rhs[pair, 128:256, 0:128] = zero
            rhs[pair, 0:64, 128:256] = jnp.where(lane, n[0:64, 0:128], 0.0).astype(BF)
            rhs[pair, 64:128, 128:256] = jnp.where(lane, 0.0, n[64:128, 0:128]).astype(BF)
            rhs[pair, 128:192, 128:256] = jnp.where(lane, n[0:64, 128:256], 0.0).astype(BF)
            rhs[pair, 192:256, 128:256] = jnp.where(lane, 0.0, n[64:128, 128:256]).astype(BF)

    def mix(lo, hi):
        def body(i, _):
            for j in range(4):
                pair = 4 * i + j
                r = pl.ds(pl.multiple_of(pair * 128, 128), 128)
                w = rhs[pair]
                for u in range(4):
                    t0 = pl.ds(u * T, T)
                    f = qf[t0, r]
                    g = jnp.dot(jnp.concatenate([f, f], axis=1), w, preferred_element_type=F32)
                    mixed[t0, r] = (g[:, 0:128] / (g[:, 128:256] + 1e-3 / 64.0)).astype(BF)
            return 0

        lax.fori_loop(lo // 4, hi // 4, body, 0)

    others = ((sib, dev(cc=1 - core)), (zs, dev(zz=zback)), (zs2, dev(zz=znext, cc=1 - core)))

    def rows(slot):
        return pl.ds(pl.multiple_of(slot * T, T), T)

    def cols(c):
        return pl.ds(pl.multiple_of(quarter * (NC * CW) + c * CW, CW), CW)

    def ocopy(c, n):
        s, target = others[n]
        return pltpu.make_async_remote_copy(
            src_ref=obuf.at[c, rows(s), :], dst_ref=out_ref.at[:, cols(c)],
            send_sem=o_ss, recv_sem=o_rs,
            device_id=target, device_id_type=MESH,
        )

    def part(c, slot):
        return jnp.dot(mixed[rows(slot), :], wbuf[c], preferred_element_type=F32).astype(BF)

    def far_tokens(c):
        obuf[c, rows(zs)] = part(c, zs)
        obuf[c, rows(zs2)] = part(c, zs2)
        ocopy(c, 1).start()
        ocopy(c, 2).start()

    def all_tokens(c):
        far = pl.ds(2 * T, 2 * T)
        obuf[c, far] = jnp.dot(mixed[far, :], wbuf[c], preferred_element_type=F32).astype(BF)
        near = pl.ds(0, 2 * T)
        obuf[c, near] = jnp.dot(mixed[near, :], wbuf[c], preferred_element_type=F32).astype(BF)
        for n in (1, 2, 0):
            ocopy(c, n).start()
        out_ref[:, cols(c)] = obuf[c, rows(me)]

    def near_tokens(c):
        obuf[c, rows(sib)] = part(c, sib)
        out_ref[:, cols(c)] = part(c, me)
        ocopy(c, 0).start()

    def o_wait():
        drain(obuf.at[pl.ds(0, 3)], o_rs)

    def finish():
        drain(obuf.at[pl.ds(0, 3)], o_ss)
        drain(wbuf.at[0, pl.ds(0, 2480), :], s_ss)
        drain(wbuf.at[:, pl.ds(0, 3840), :], w_ss)
        drain(qbuf.at[pl.ds(0, 3)], q_ss)

    plan = [
        ("start", start),
        ("theirs", theirs),
        ("mine", mine),
        ("z_ready", z_ready),
        ("qlink0", lambda: qlink(0, 2)),
        ("chip_sum", chip_sum),
        ("qlink1", lambda: qlink(2, 6)),
        ("e1_0", lambda: e1(0)),
        ("far_ready", far_ready),
        ("near_sum", near_sum),
        ("qlink2", lambda: qlink(6, 12)),
        ("e1_1", lambda: e1(1)),
        ("e1_2", lambda: e1(2)),
        ("qf_me", lambda: qfeat(me, 0, QP)),
        ("e1_3", lambda: e1(3)),
        ("qsib", lambda: qwait(0, QP)),
        ("qf_sib", lambda: qfeat(sib, 0, QP)),
        ("far_sum", far_sum),
        ("qlink3", lambda: qlink(12, QP)),
        ("e3_0", lambda: e3(0)),
        ("qrelay1", lambda: qrelay(0)),
        ("qf_zs", lambda: qfeat(zs, 0, 8)),
        ("e3_1", lambda: e3(1)),
        ("e4a_0", lambda: e4(0, 0)),
        ("qtwin1", lambda: qwait(3, 8)),
        ("qf_tw", lambda: qfeat(zs2, 0, 8)),
        ("e4a_1", lambda: e4(1, 0)),
        ("far_back", far_back),
        ("qrelay2", lambda: qrelay(1)),
        ("qf_zs2", lambda: qfeat(zs, 8, QP)),
        ("e3_2", lambda: e3(2)),
        ("twin0", lambda: twin(0)),
        ("qtwin2", lambda: qwait(4, 8)),
        ("qf_tw2", lambda: qfeat(zs2, 8, QP)),
        ("e3_3", lambda: e3(3)),
        ("e4b_0", lambda: e4(0, 1)),
        ("take3", lambda: take(3)),
        ("e4a_2", lambda: e4(2, 0)),
        ("take1", lambda: take(1)),
        ("e4b_1", lambda: e4(1, 1)),
        ("twin3", lambda: twin(3)),
        ("twin1", lambda: twin(1)),
        ("take2", lambda: take(2)),
        ("e4a_3", lambda: e4(3, 0)),
        ("twin2", lambda: twin(2)),
        ("mix0", lambda: mix(0, 16)),
        ("e4b_2", lambda: e4(2, 1)),
        ("mix1", lambda: mix(16, 32)),
        ("e4b_3", lambda: e4(3, 1)),
        ("e5_0", lambda: e5(0)),
        ("pr_0", lambda: all_tokens(0)),
        ("e5_1", lambda: e5(1)),
        ("pr_1", lambda: all_tokens(1)),
        ("e5_2", lambda: e5(2)),
        ("pr_2", lambda: all_tokens(2)),
        ("e5_3", lambda: e5(3)),
        ("prf_3", lambda: far_tokens(3)),
        ("prn_3", lambda: near_tokens(3)),
        ("o_wait", o_wait),
        ("finish", finish),
    ]
    for name, step in plan:
        step()


def shards(asked_for, offered, contents, out_weight):
    def view(a):
        return jnp.transpose(a, (0, 2, 3, 1)).reshape(D, T)

    dma = pltpu.SemaphoreType.DMA
    hbm = pl.BlockSpec(memory_space=pl.ANY)
    out = pl.pallas_call(
        kernel,
        out_shape=pltpu.VMEM((T, D), BF),
        in_specs=[hbm] * 4,
        out_specs=pl.BlockSpec(memory_space=pltpu.VMEM),
        scratch_shapes=[
            pltpu.VMEM((NC, D, CW), BF),
            pltpu.VMEM((4, D, T), BF),
            pltpu.VMEM((D, T), BF),
            pltpu.VMEM((D, T), BF),
            pltpu.VMEM((4 * T, D), BF),
            pltpu.VMEM((4, 4, SR, 128), F32),
            pltpu.VMEM((4, 4, SR, 128), BF),
            pltpu.VMEM((4, 4, SR, 128), BF),
            pltpu.VMEM((4, 4, SR, 128), BF),
            pltpu.VMEM((3, 4, SR, 128), BF),
            pltpu.VMEM((4, SR, 128), F32),
            pltpu.VMEM((4, SR, 128), BF),
            pltpu.VMEM((3, SR, 128), BF),
            pltpu.VMEM((2, 4, 4, SR, 128), BF),
            pltpu.VMEM((32, 256, 256), BF),
            pltpu.VMEM((4 * T, D), BF),
            pltpu.VMEM((NC, 4 * T, CW), BF),
            dma((NC + 3,)), dma, dma((NC, 5)), dma, dma((5,)), dma, dma, dma, dma, dma, dma((3,)), dma((4,)), dma, dma,
            *[pltpu.SemaphoreType.REGULAR] * 4,
        ],
        compiler_params=pltpu.CompilerParams(
            collective_id=0, has_side_effects=True, vmem_limit_bytes=56 * 1024 * 1024
        ),
        name="attend_project",
    )(view(asked_for), view(offered), view(contents), out_weight)
    return out.reshape(1, T, D)


def solution(mesh):
    in_specs = (
        P("batch", "ctx", None, None),
        P("batch", "ctx", None, None),
        P("batch", "ctx", None, None),
        P("batch", None),
    )
    return jax.shard_map(shards, mesh=mesh, in_specs=in_specs, out_specs=P("batch", "ctx", None), check_vma=False)
```

```python
import jax
import jax.numpy as jnp
from jax import lax
from jax.experimental import pallas as pl
from jax.experimental.pallas import tpu as pltpu
from jax.sharding import PartitionSpec as P

BF = jnp.bfloat16
F32 = jnp.float32
MESH = pl.DeviceIdType.MESH
D = 4096
T = 128
NC = 4
CW = 256
CHUNKS = ((0, 0, 256), (1, 0, 256), (2, 0, 256), (3, 0, 256))
LEFT = (0, 1, 0, 1)
SR = 80
QP = 16


def feature(x):
    return jnp.log(1.0 + jnp.exp(x.astype(F32))).astype(BF)


def pack(s):
    m = s[64:72]
    hi = m.astype(BF).astype(F32)
    return jnp.concatenate([s[0:64], hi, m - hi], axis=0).astype(BF)


def unpack(b):
    f = b.astype(F32)
    m = f[64:72] + f[72:80]
    return jnp.concatenate([f[0:64], m, m], axis=0)


def kernel(
    q_hbm, k_hbm, v_hbm, w_hbm, out_ref,
    wbuf, qbuf, kbuf, vbuf, qf, st, dsend, drecv, r1s, r1r, acc, r2s, r2r, gat, rhs, mixed, obuf,
    lsem, w_ss, w_rs, q_ss, q_rs, s_ss, d_rs, r1_rs, r2_rs, g2_rs, g1_rs, gd_rs, o_ss, o_rs, semA, semB, semP, semZ,
):
    b = lax.axis_index("batch")
    t = lax.axis_index("ctx")
    y, x = b // 4, b % 4
    z, core = t // 2, t % 2
    zp = z % 2
    quarter = 2 * zp + core
    me, sib, zs, zs2 = core, 1 - core, 2 + core, 3 - core
    znext = (z + 2 * core + 15) % 16
    zback = (z - 2 * core + 17) % 16
    cls, m0 = z % 4, z // 4

    def dev(dy=0, dx=0, zz=None, cc=None):
        zz = z if zz is None else zz
        cc = core if cc is None else cc
        return (((y + dy) % 4) * 4 + (x + dx) % 4, zz * 2 + cc)

    def zdev(dz):
        return dev(zz=(z + dz + 16) % 16)

    lw = [
        pltpu.make_async_copy(
            w_hbm.at[:, pl.ds(pl.multiple_of(quarter * (NC * CW) + c * CW, CW), CW)],
            wbuf.at[c, pl.ds(pl.multiple_of(b * 256, 256), 256), :],
            lsem.at[c],
        )
        for c in range(NC)
    ]
    lk = pltpu.make_async_copy(k_hbm, kbuf, lsem.at[NC])
    lv = pltpu.make_async_copy(v_hbm, vbuf, lsem.at[NC + 1])
    lq = pltpu.make_async_copy(q_hbm, qbuf.at[me], lsem.at[NC + 2])
    for c in lw:
        c.start()

    barrier = pltpu.get_barrier_semaphore()

    def tell(sem, d):
        pl.semaphore_signal(sem, inc=1, device_id=d, device_id_type=MESH)

    twin_core = dev(cc=1 - core)
    for dy, dx in ((0, 1), (0, 3), (1, 0), (3, 0)):
        tell(barrier, dev(dy=dy, dx=dx, cc=0))
    for dz in (1, -1, 2, -2):
        tell(barrier, dev(zz=(z + dz + 16) % 16, cc=1))

    @pl.when(core == 1)
    def _():
        tell(barrier, twin_core)

    for c in (lk, lv, lq):
        c.start()

    @pl.when(core == 0)
    def _():
        pl.semaphore_wait(barrier, 9)
        tell(semP, twin_core)

    @pl.when(core == 1)
    def _():
        pl.semaphore_wait(semP, 1)

    def z_ready():
        @pl.when(core == 1)
        def _():
            pl.semaphore_wait(barrier, 8)
            tell(semZ, twin_core)

        @pl.when(core == 0)
        def _():
            pl.semaphore_wait(semZ, 1)

        for d in (zdev(2), zdev(-2)):
            tell(semA, d)

    def drain(ref, sem):
        pltpu.make_async_copy(ref, ref, sem).wait()

    groups = {(1, 0): 0, (3, 0): 0, (2, 0): 1, (0, 3): 2, (3, 1): 2, (1, 3): 3, (2, 1): 3}

    def wsend(c, h, dp, ds, tp, ts):
        dy, dx = (ds, dp) if h == 0 else (dp, ds)
        ty, tx = (ts, tp) if h == 0 else (tp, ts)
        blk = ((y + dy + 4) % 4) * 4 + (x + dx + 4) % 4
        buf, lo, width = CHUNKS[c]
        ref = wbuf.at[buf, pl.ds(pl.multiple_of(blk * 256 + h * 128, 128), 128), pl.ds(lo, width)]
        pltpu.make_async_remote_copy(
            src_ref=ref, dst_ref=ref, send_sem=w_ss,
            recv_sem=w_rs.at[c, groups.get(((dp - tp) % 4, (ds - ts) % 4), 4)],
            device_id=dev(dy=ty % 4, dx=tx % 4), device_id_type=MESH,
        ).start()

    def wwait(c, g):
        buf, lo, width = CHUNKS[c]
        drain(wbuf.at[buf, pl.ds(0, (4, 2, 4, 4, 16)[g] * 128), pl.ds(lo, width)], w_rs.at[c, g])

    def e0(c):
        for h in (0, 1):
            for tp, ts in ((1, 0), (-1, 0), (0, 1), (0, -1)):
                wsend(c, h, 0, 0, tp, ts)

    def e1(c):
        wwait(c, 0)
        for h in (0, 1):
            wsend(c, h, *(((-1, 0, 1, 0), (1, 0, -1, 0))[LEFT[c]]))
            for dp in (-1, 1):
                wsend(c, h, dp, 0, 0, 1)
                wsend(c, h, dp, 0, 0, -1)

    def e3(c):
        wwait(c, 1)
        for h in (0, 1):
            wsend(c, h, 2, 0, 0, 1)
            wsend(c, h, 2, 0, 0, -1)

    def e4(c, late):
        wwait(c, 2 + late)
        for h in (0, 1):
            for dp, ds in (((0, -1), (-1, 1)), ((1, -1), (2, 1)))[late]:
                wsend(c, h, dp, ds, 0, -ds)

    def e5(c):
        wwait(c, 4)

    qr = D // QP

    def qcopy(slot, to, i, n, target, sem):
        r = pl.ds(i * qr, n * qr)
        pltpu.make_async_remote_copy(
            src_ref=qbuf.at[slot, r, :], dst_ref=qbuf.at[to, r, :], send_sem=q_ss, recv_sem=q_rs.at[sem],
            device_id=target, device_id_type=MESH,
        ).start()

    def qwait(sem, n):
        drain(qbuf.at[0, pl.ds(0, n * qr), :], q_rs.at[sem])

    def qlink(lo, hi):
        for i in range(lo, hi):
            qcopy(me, zs, i, 1, dev(zz=znext), 1 + i // 8)

    def qrelay(half):
        qwait(1 + half, 8)
        qcopy(zs, zs, 8 * half, 8, twin_core, 3 + half)

    def qfeat(slot, lo, hi):
        def body(i, _):
            r = pl.ds(pl.multiple_of(i * 128, 128), 128)
            qf[pl.ds(pl.multiple_of(slot * T, T), T), r] = feature(qbuf[slot, r, :]).T
            return 0
        lax.fori_loop(lo * (32 // QP), hi * (32 // QP), body, 0, unroll=2)

    def start():
        for c in range(NC):
            lw[c].wait()
            e0(c)
        lq.wait()
        qcopy(me, me, 0, QP, twin_core, 0)

    lane = lax.broadcasted_iota(jnp.int32, (64, 128), 1) < 64
    nt = (((1,), (1,)), ((), ()))

    def partial(half, i):
        k, m = i // 4, i % 4
        r = pl.ds(pl.multiple_of((16 * half + 4 * m + k) * 128, 128), 128)
        kf = feature(kbuf[r, :])
        g = lax.dot_general(kf, vbuf[r, :], nt, preferred_element_type=F32)
        n = lax.dot_general(jnp.ones((16, 128), BF), kf, nt, preferred_element_type=F32)
        return k, m, jnp.concatenate([jnp.where(lane, g[0:64], g[64:128]), n], axis=0)

    dcopy = pltpu.make_async_remote_copy(
        src_ref=dsend, dst_ref=drecv, send_sem=s_ss, recv_sem=d_rs, device_id=dev(cc=1 - core), device_id_type=MESH
    )

    def theirs():
        lk.wait()
        lv.wait()

        def body(i, _):
            k, m, s = partial(1 - core, i)
            dsend[k, m] = pack(s)
            return 0

        lax.fori_loop(0, 16, body, 0, unroll=4)
        dcopy.start()

    def mine():
        def body(i, _):
            k, m, s = partial(core, i)
            st[k, m] = s
            return 0

        lax.fori_loop(0, 16, body, 0, unroll=4)

    def r1copy(n):
        dz, slot, lo, cnt = ((1, 0, 0, 4), (-1, 1, 0, 4), (2, 2, 0, 2), (-2, 2, 2, 2))[n]
        k = (z + dz + 16) % 4
        return pltpu.make_async_remote_copy(
            src_ref=r1s.at[k, pl.ds(lo, cnt)], dst_ref=r1r.at[slot, pl.ds(lo, cnt)],
            send_sem=s_ss, recv_sem=r1_rs, device_id=zdev(dz), device_id_type=MESH,
        )

    def chip_sum():
        dcopy.wait_recv()

        def body(i, _):
            k, m = i // 4, i % 4
            s = st[k, m] + unpack(drecv[k, m])
            st[k, m] = s
            r1s[k, m] = pack(s)
            return 0

        lax.fori_loop(0, 16, body, 0, unroll=4)
        for n in (2, 3, 0, 1):
            r1copy(n).start()

    def far_ready():
        pl.semaphore_wait(semA, 2)
        for d in (zdev(4), zdev(-4)):
            pl.semaphore_signal(semB, inc=1, device_id=d, device_id_type=MESH)

    def r2copy(r):
        return pltpu.make_async_remote_copy(
            src_ref=r2s.at[(m0 + r) % 4], dst_ref=r2r.at[r - 1],
            send_sem=s_ss, recv_sem=r2_rs, device_id=zdev(4 * r), device_id_type=MESH,
        )

    def near_sum():
        drain(r1r, r1_rs)

        def body(m, _):
            s = st[cls, m] + unpack(r1r[0, m]) + unpack(r1r[1, m]) + unpack(r1r[2, m])
            acc[m] = s
            r2s[m] = pack(s)
            return 0

        lax.fori_loop(0, 4, body, 0)
        pl.semaphore_wait(semB, 2)
        for r in (2, 1, 3):
            r2copy(r).start()

    def g2copy(r):
        ref = gat.at[core, cls, m0]
        return pltpu.make_async_remote_copy(
            src_ref=ref, dst_ref=ref, send_sem=s_ss, recv_sem=g2_rs,
            device_id=zdev(4 * r), device_id_type=MESH,
        )

    def far_sum():
        drain(r2r, r2_rs)
        total = (acc[m0] + unpack(r2r[0]) + unpack(r2r[1]) + unpack(r2r[2])) * (1.0 / (32 * T))
        gat[core, cls, m0] = pack(total)
        for r in (2, 1, 3):
            g2copy(r).start()

    def g1copy(n):
        dz, lo, cnt = ((1, 0, 4), (-1, 0, 4), (2, 0, 2), (-2, 2, 2))[n]
        ref = gat.at[core, cls, pl.ds(lo, cnt)]
        return pltpu.make_async_remote_copy(
            src_ref=ref, dst_ref=ref, send_sem=s_ss, recv_sem=g1_rs.at[min(n, 2)],
            device_id=zdev(dz), device_id_type=MESH,
        )

    def gdcopy(dk):
        ref = gat.at[core, (cls + dk) % 4]
        return pltpu.make_async_remote_copy(
            src_ref=ref, dst_ref=ref, send_sem=s_ss, recv_sem=gd_rs.at[dk],
            device_id=dev(cc=1 - core), device_id_type=MESH,
        )

    def far_back():
        drain(r2r, g2_rs)
        for n in (2, 3, 0, 1):
            g1copy(n).start()
        gdcopy(0).start()
        prep(0, core, cls)

    order = ((core, 0), (1 - core, 0), (core, 3), (core, 1), (1 - core, 3), (1 - core, 1), (core, 2), (1 - core, 2))

    def take(n, dk):
        drain(gat.at[core, cls], g1_rs.at[{3: 0, 1: 1, 2: 2}[dk]])
        gdcopy(dk).start()
        prep(n, core, (cls + dk) % 4)
        mix(n - 1)

    def twin(n, dk, before=True):
        gdcopy(dk).wait_recv()
        prep(n, 1 - core, (cls + dk) % 4)
        if before:
            mix(n - 1)

    def prep(step, half, k):
        row = lax.broadcasted_iota(jnp.int32, (16, 256), 0)
        col = lax.broadcasted_iota(jnp.int32, (16, 256), 1) // 128
        pick = jnp.where(row == 8 * col, 1.0 / 64.0, 0.0).astype(BF)
        zero = jnp.zeros((128, 128), BF)
        for m in range(4):
            s = gat[half, k, m]
            a = s[0:64].astype(F32)
            n = lax.dot_general(s[64:80], pick, (((0,), (0,)), ((), ())), preferred_element_type=F32)
            at = 4 * step + m
            rhs[at, 0:64, 0:128] = jnp.where(lane, a, 0.0).astype(BF)
            rhs[at, 64:128, 0:128] = jnp.where(lane, 0.0, a).astype(BF)
            rhs[at, 128:256, 0:128] = zero
            rhs[at, 0:64, 128:256] = jnp.where(lane, n[0:64, 0:128], 0.0).astype(BF)
            rhs[at, 64:128, 128:256] = jnp.where(lane, 0.0, n[64:128, 0:128]).astype(BF)
            rhs[at, 128:192, 128:256] = jnp.where(lane, n[0:64, 128:256], 0.0).astype(BF)
            rhs[at, 192:256, 128:256] = jnp.where(lane, 0.0, n[64:128, 128:256]).astype(BF)

    def mix(step):
        half, dk = order[step]
        k = (cls + dk) % 4
        for m in range(4):
            r = pl.ds(pl.multiple_of((16 * half + 4 * m + k) * 128, 128), 128)
            w = rhs[4 * step + m]
            for u in range(4):
                t0 = pl.ds(u * T, T)
                f = qf[t0, r]
                g = jnp.dot(jnp.concatenate([f, f], axis=1), w, preferred_element_type=F32)
                mixed[t0, r] = (g[:, 0:128] / (g[:, 128:256] + 1e-3 / 64.0)).astype(BF)

    def rows(slot):
        return pl.ds(pl.multiple_of(slot * T, T), T)

    def cols(c):
        buf, lo, width = CHUNKS[c]
        return pl.ds(pl.multiple_of(quarter * (NC * CW) + buf * CW + lo, 128), width)

    def ocopy(c, slot, target):
        buf, lo, width = CHUNKS[c]
        return pltpu.make_async_remote_copy(
            src_ref=obuf.at[buf, rows(slot), pl.ds(lo, width)], dst_ref=out_ref.at[:, cols(c)],
            send_sem=o_ss, recv_sem=o_rs, device_id=target, device_id_type=MESH,
        )

    znear = {2: dev(zz=(z + 1) % 16, cc=0), 3: dev(zz=(z + 15) % 16, cc=1)}

    def part(c, r, k=pl.ds(0, D)):
        buf, lo, width = CHUNKS[c]
        return jnp.dot(mixed[r, k], wbuf[buf, k, lo : lo + width], preferred_element_type=F32)

    def put(c, r, value):
        buf, lo, width = CHUNKS[c]
        obuf[buf, r, lo : lo + width] = value.astype(BF)

    def own(c):
        buf, lo, width = CHUNKS[c]
        ocopy(c, sib, twin_core).start()
        out_ref[:, cols(c)] = obuf[buf, rows(me), lo : lo + width]

    def project(c):
        for first in (2, 0):
            r = pl.ds(first * T, 2 * T)
            put(c, r, part(c, r))
        ocopy(c, 2, znear[2]).start()
        ocopy(c, 3, znear[3]).start()
        own(c)

    def far_tokens(c, halves):
        for slot in (2, 3):
            r = pl.ds(slot * T, T)
            if halves:
                put(c, r, part(c, r, pl.ds(0, D // 2)) + part(c, r, pl.ds(D // 2, D // 2)))
                ocopy(c, slot, znear[slot]).start()
            else:
                put(c, r, part(c, r))
        if not halves:
            for slot in (2, 3):
                ocopy(c, slot, znear[slot]).start()

    def near_tokens(c):
        for slot in (0, 1):
            r = pl.ds(slot * T, T)
            put(c, r, part(c, r))
        own(c)

    def o_wait():
        drain(obuf.at[pl.ds(0, 3)], o_rs)

    def finish():
        drain(obuf.at[pl.ds(0, 3)], o_ss)
        drain(wbuf.at[0, pl.ds(0, 2480), :], s_ss)
        drain(wbuf.at[:, pl.ds(0, 3840), :], w_ss)
        drain(qbuf.at[pl.ds(0, 3)], q_ss)

    plan = [
        ("start", start),
        ("theirs", theirs),
        ("mine", mine),
        ("z_ready", z_ready),
        ("qlink0", lambda: qlink(0, 2)),
        ("chip_sum", chip_sum),
        ("qlink1", lambda: qlink(2, 6)),
        ("e1_0", lambda: e1(0)),
        ("far_ready", far_ready),
        ("e1_1", lambda: e1(1)),
        ("near_sum", near_sum),
        ("qlink2", lambda: qlink(6, 12)),
        ("e1_2", lambda: e1(2)),
        ("qf_me", lambda: qfeat(me, 0, QP)),
        ("e1_3", lambda: e1(3)),
        ("qsib", lambda: qwait(0, QP)),
        ("qf_sib", lambda: qfeat(sib, 0, QP)),
        ("far_sum", far_sum),
        ("qlink3", lambda: qlink(12, QP)),
        ("e3_0", lambda: e3(0)),
        ("qrelay1", lambda: qrelay(0)),
        ("qf_zs", lambda: qfeat(zs, 0, 8)),
        ("e3_1", lambda: e3(1)),
        ("e4a_0", lambda: e4(0, 0)),
        ("qtwin1", lambda: qwait(3, 8)),
        ("qf_tw", lambda: qfeat(zs2, 0, 8)),
        ("e4a_1", lambda: e4(1, 0)),
        ("e3_2", lambda: e3(2)),
        ("far_back", far_back),
        ("qrelay2", lambda: qrelay(1)),
        ("qf_zs2", lambda: qfeat(zs, 8, QP)),
        ("twin0", lambda: twin(1, 0, before=False)),
        ("e4b_0", lambda: e4(0, 1)),
        ("qtwin2", lambda: qwait(4, 8)),
        ("e3_3", lambda: e3(3)),
        ("qf_tw2", lambda: qfeat(zs2, 8, QP)),
        ("e4b_1", lambda: e4(1, 1)),
        ("mix0", lambda: mix(0)),
        ("e4a_2", lambda: e4(2, 0)),
        ("take3", lambda: take(2, 3)),
        ("take1", lambda: take(3, 1)),
        ("e4a_3", lambda: e4(3, 0)),
        ("twin3", lambda: twin(4, 3)),
        ("e4b_2", lambda: e4(2, 1)),
        ("twin1", lambda: twin(5, 1)),
        ("take2", lambda: take(6, 2)),
        ("twin2", lambda: twin(7, 2)),
        ("e4b_3", lambda: e4(3, 1)),
        ("mix7", lambda: mix(7)),
        ("e5_0", lambda: e5(0)),
        ("pr_0", lambda: project(0)),
        ("e5_1", lambda: e5(1)),
        ("pr_1", lambda: project(1)),
        ("e5_2", lambda: e5(2)),
        ("prf_2", lambda: far_tokens(2, False)),
        ("e5_3", lambda: e5(3)),
        ("prf_3", lambda: far_tokens(3, True)),
        ("prn_2", lambda: near_tokens(2)),
        ("prn_3", lambda: near_tokens(3)),
        ("o_wait", o_wait),
        ("finish", finish),
    ]
    for name, step in plan:
        step()


def shards(asked_for, offered, contents, out_weight):
    def view(a):
        return jnp.transpose(a, (0, 2, 3, 1)).reshape(D, T)

    dma = pltpu.SemaphoreType.DMA
    hbm = pl.BlockSpec(memory_space=pl.ANY)
    out = pl.pallas_call(
        kernel,
        out_shape=pltpu.VMEM((T, D), BF),
        in_specs=[hbm] * 4,
        out_specs=pl.BlockSpec(memory_space=pltpu.VMEM),
        scratch_shapes=[
            pltpu.VMEM((NC, D, CW), BF),
            pltpu.VMEM((4, D, T), BF),
            pltpu.VMEM((D, T), BF),
            pltpu.VMEM((D, T), BF),
            pltpu.VMEM((4 * T, D), BF),
            pltpu.VMEM((4, 4, SR, 128), F32),
            pltpu.VMEM((4, 4, SR, 128), BF),
            pltpu.VMEM((4, 4, SR, 128), BF),
            pltpu.VMEM((4, 4, SR, 128), BF),
            pltpu.VMEM((3, 4, SR, 128), BF),
            pltpu.VMEM((4, SR, 128), F32),
            pltpu.VMEM((4, SR, 128), BF),
            pltpu.VMEM((3, SR, 128), BF),
            pltpu.VMEM((2, 4, 4, SR, 128), BF),
            pltpu.VMEM((32, 256, 256), BF),
            pltpu.VMEM((4 * T, D), BF),
            pltpu.VMEM((NC, 4 * T, CW), BF),
            dma((NC + 3,)), dma, dma((NC, 5)), dma, dma((5,)), dma, dma, dma, dma, dma, dma((3,)), dma((4,)), dma, dma,
            *[pltpu.SemaphoreType.REGULAR] * 4,
        ],
        compiler_params=pltpu.CompilerParams(
            collective_id=0, has_side_effects=True, vmem_limit_bytes=56 * 1024 * 1024
        ),
        name="attend_project",
    )(view(asked_for), view(offered), view(contents), out_weight)
    return out.reshape(1, T, D)


def solution(mesh):
    in_specs = (
        P("batch", "ctx", None, None),
        P("batch", "ctx", None, None),
        P("batch", "ctx", None, None),
        P("batch", None),
    )
    return jax.shard_map(shards, mesh=mesh, in_specs=in_specs, out_specs=P("batch", "ctx", None), check_vma=False)
```

```python
import jax
import jax.numpy as jnp
from jax import lax
from jax.experimental import pallas as pl
from jax.experimental.pallas import tpu as pltpu
from jax.sharding import PartitionSpec as P

BF = jnp.bfloat16
F32 = jnp.float32
MESH = pl.DeviceIdType.MESH
D = 4096
T = 128
NC = 4
CW = 256
CHUNKS = ((0, 0, 256), (1, 0, 256), (2, 0, 256), (3, 0, 256))
LEFT = (0, 1, 0, 1)
SR = 80
QP = 16


def feature(x):
    return jnp.log(1.0 + jnp.exp(x.astype(F32))).astype(BF)


def pack(s):
    m = s[64:72]
    hi = m.astype(BF).astype(F32)
    return jnp.concatenate([s[0:64], hi, m - hi], axis=0).astype(BF)


def unpack(b):
    f = b.astype(F32)
    m = f[64:72] + f[72:80]
    return jnp.concatenate([f[0:64], m, m], axis=0)


def kernel(
    q_hbm, k_hbm, v_hbm, w_hbm, out_ref,
    wbuf, qbuf, kbuf, vbuf, qf, st, dsend, drecv, r1s, r1r, acc, r2s, r2r, gat, rhs, mixed, obuf,
    lsem, w_ss, w_rs, q_ss, q_rs, s_ss, d_rs, r1_rs, r2_rs, g2_rs, g1_rs, gd_rs, o_ss, o_rs, semA, semB, semP, semZ,
):
    b = lax.axis_index("batch")
    t = lax.axis_index("ctx")
    y, x = b // 4, b % 4
    z, core = t // 2, t % 2
    zp = z % 2
    quarter = 2 * zp + core
    me, sib, zs, zs2 = core, 1 - core, 2 + core, 3 - core
    znext = (z + 2 * core + 15) % 16
    zback = (z - 2 * core + 17) % 16
    cls, m0 = z % 4, z // 4

    def dev(dy=0, dx=0, zz=None, cc=None):
        zz = z if zz is None else zz
        cc = core if cc is None else cc
        return (((y + dy) % 4) * 4 + (x + dx) % 4, zz * 2 + cc)

    def zdev(dz):
        return dev(zz=(z + dz + 16) % 16)

    lw = [
        pltpu.make_async_copy(
            w_hbm.at[:, pl.ds(pl.multiple_of(quarter * (NC * CW) + c * CW, CW), CW)],
            wbuf.at[c, pl.ds(pl.multiple_of(b * 256, 256), 256), :],
            lsem.at[c],
        )
        for c in range(NC)
    ]
    lk = pltpu.make_async_copy(k_hbm, kbuf, lsem.at[NC])
    lv = pltpu.make_async_copy(v_hbm, vbuf, lsem.at[NC + 1])
    lq = pltpu.make_async_copy(q_hbm, qbuf.at[me], lsem.at[NC + 2])
    for c in lw:
        c.start()

    barrier = pltpu.get_barrier_semaphore()

    def tell(sem, d):
        pl.semaphore_signal(sem, inc=1, device_id=d, device_id_type=MESH)

    twin_core = dev(cc=1 - core)
    for dy, dx in ((0, 1), (0, 3), (1, 0), (3, 0)):
        tell(barrier, dev(dy=dy, dx=dx, cc=0))
    for dz in (1, -1, 2, -2):
        tell(barrier, dev(zz=(z + dz + 16) % 16, cc=1))

    @pl.when(core == 1)
    def _():
        tell(barrier, twin_core)

    for c in (lk, lv, lq):
        c.start()

    @pl.when(core == 0)
    def _():
        pl.semaphore_wait(barrier, 9)
        tell(semP, twin_core)

    @pl.when(core == 1)
    def _():
        pl.semaphore_wait(semP, 1)

    def z_ready():
        @pl.when(core == 1)
        def _():
            pl.semaphore_wait(barrier, 8)
            tell(semZ, twin_core)

        @pl.when(core == 0)
        def _():
            pl.semaphore_wait(semZ, 1)

        for d in (zdev(2), zdev(-2)):
            tell(semA, d)

    def drain(ref, sem):
        pltpu.make_async_copy(ref, ref, sem).wait()

    groups = {(1, 0): 0, (3, 0): 0, (2, 0): 1, (0, 3): 2, (3, 1): 2, (1, 3): 2, (2, 1): 3}

    def wsend(c, h, dp, ds, tp, ts):
        dy, dx = (ds, dp) if h == 0 else (dp, ds)
        ty, tx = (ts, tp) if h == 0 else (tp, ts)
        blk = ((y + dy + 4) % 4) * 4 + (x + dx + 4) % 4
        buf, lo, width = CHUNKS[c]
        ref = wbuf.at[buf, pl.ds(pl.multiple_of(blk * 256 + h * 128, 128), 128), pl.ds(lo, width)]
        pltpu.make_async_remote_copy(
            src_ref=ref, dst_ref=ref, send_sem=w_ss,
            recv_sem=w_rs.at[c, groups.get(((dp - tp) % 4, (ds - ts) % 4), 4)],
            device_id=dev(dy=ty % 4, dx=tx % 4), device_id_type=MESH,
        ).start()

    def wwait(c, g):
        buf, lo, width = CHUNKS[c]
        drain(wbuf.at[buf, pl.ds(0, (4, 2, 6, 2, 16)[g] * 128), pl.ds(lo, width)], w_rs.at[c, g])

    def e0(c):
        for h in (0, 1):
            for tp, ts in ((1, 0), (-1, 0), (0, 1), (0, -1)):
                wsend(c, h, 0, 0, tp, ts)

    def e1(c):
        wwait(c, 0)
        for h in (0, 1):
            wsend(c, h, *(((-1, 0, 1, 0), (1, 0, -1, 0))[LEFT[c]]))
            for dp in (-1, 1):
                wsend(c, h, dp, 0, 0, 1)
                wsend(c, h, dp, 0, 0, -1)

    def e3(c):
        wwait(c, 1)
        for h in (0, 1):
            wsend(c, h, 2, 0, 0, 1)
            wsend(c, h, 2, 0, 0, -1)

    def e4(c, late):
        wwait(c, 2 + late)
        for h in (0, 1):
            for dp, ds in (((0, -1), (-1, 1), (1, -1)), ((2, 1),))[late]:
                wsend(c, h, dp, ds, 0, -ds)

    def e5(c):
        wwait(c, 4)

    qr = D // QP

    def qcopy(slot, to, i, n, target, sem):
        r = pl.ds(i * qr, n * qr)
        pltpu.make_async_remote_copy(
            src_ref=qbuf.at[slot, r, :], dst_ref=qbuf.at[to, r, :], send_sem=q_ss, recv_sem=q_rs.at[sem],
            device_id=target, device_id_type=MESH,
        ).start()

    def qwait(sem, n):
        drain(qbuf.at[0, pl.ds(0, n * qr), :], q_rs.at[sem])

    def qlink(lo, hi):
        for i in range(lo, hi):
            qcopy(me, zs, i, 1, dev(zz=znext), 1 + i // 8)

    def qrelay(half):
        qwait(1 + half, 8)
        qcopy(zs, zs, 8 * half, 8, twin_core, 3 + half)

    def qfeat(slot, lo, hi):
        def body(i, _):
            r = pl.ds(pl.multiple_of(i * 128, 128), 128)
            qf[pl.ds(pl.multiple_of(slot * T, T), T), r] = feature(qbuf[slot, r, :]).T
            return 0
        lax.fori_loop(lo * (32 // QP), hi * (32 // QP), body, 0, unroll=2)

    def start():
        for c in range(NC):
            lw[c].wait()
            e0(c)
        lq.wait()
        qcopy(me, me, 0, QP, twin_core, 0)

    lane = lax.broadcasted_iota(jnp.int32, (64, 128), 1) < 64
    nt = (((1,), (1,)), ((), ()))

    def partial(half, i):
        k, m = i // 4, i % 4
        r = pl.ds(pl.multiple_of((16 * half + 4 * m + k) * 128, 128), 128)
        kf = feature(kbuf[r, :])
        g = lax.dot_general(kf, vbuf[r, :], nt, preferred_element_type=F32)
        n = lax.dot_general(jnp.ones((16, 128), BF), kf, nt, preferred_element_type=F32)
        return k, m, jnp.concatenate([jnp.where(lane, g[0:64], g[64:128]), n], axis=0)

    dcopy = pltpu.make_async_remote_copy(
        src_ref=dsend, dst_ref=drecv, send_sem=s_ss, recv_sem=d_rs, device_id=dev(cc=1 - core), device_id_type=MESH
    )

    def theirs():
        lk.wait()
        lv.wait()

        def body(i, _):
            k, m, s = partial(1 - core, i)
            dsend[k, m] = pack(s)
            return 0

        lax.fori_loop(0, 16, body, 0, unroll=4)
        dcopy.start()

    def mine():
        def body(i, _):
            k, m, s = partial(core, i)
            st[k, m] = s
            return 0

        lax.fori_loop(0, 16, body, 0, unroll=4)

    def r1copy(n):
        dz, slot, lo, cnt = ((1, 0, 0, 4), (-1, 1, 0, 4), (2, 2, 0, 2), (-2, 2, 2, 2))[n]
        k = (z + dz + 16) % 4
        return pltpu.make_async_remote_copy(
            src_ref=r1s.at[k, pl.ds(lo, cnt)], dst_ref=r1r.at[slot, pl.ds(lo, cnt)],
            send_sem=s_ss, recv_sem=r1_rs, device_id=zdev(dz), device_id_type=MESH,
        )

    def chip_sum():
        dcopy.wait_recv()

        def body(i, _):
            k, m = i // 4, i % 4
            s = st[k, m] + unpack(drecv[k, m])
            st[k, m] = s
            r1s[k, m] = pack(s)
            return 0

        lax.fori_loop(0, 16, body, 0, unroll=4)
        for n in (2, 3, 0, 1):
            r1copy(n).start()

    def far_ready():
        pl.semaphore_wait(semA, 2)
        for d in (zdev(4), zdev(-4)):
            pl.semaphore_signal(semB, inc=1, device_id=d, device_id_type=MESH)

    def r2copy(r):
        return pltpu.make_async_remote_copy(
            src_ref=r2s.at[(m0 + r) % 4], dst_ref=r2r.at[r - 1],
            send_sem=s_ss, recv_sem=r2_rs, device_id=zdev(4 * r), device_id_type=MESH,
        )

    def near_sum():
        drain(r1r, r1_rs)

        def body(m, _):
            s = st[cls, m] + unpack(r1r[0, m]) + unpack(r1r[1, m]) + unpack(r1r[2, m])
            acc[m] = s
            r2s[m] = pack(s)
            return 0

        lax.fori_loop(0, 4, body, 0)
        pl.semaphore_wait(semB, 2)
        for r in (2, 1, 3):
            r2copy(r).start()

    def g2copy(r):
        ref = gat.at[core, cls, m0]
        return pltpu.make_async_remote_copy(
            src_ref=ref, dst_ref=ref, send_sem=s_ss, recv_sem=g2_rs,
            device_id=zdev(4 * r), device_id_type=MESH,
        )

    def far_sum():
        drain(r2r, r2_rs)
        total = (acc[m0] + unpack(r2r[0]) + unpack(r2r[1]) + unpack(r2r[2])) * (1.0 / (32 * T))
        gat[core, cls, m0] = pack(total)
        for r in (2, 1, 3):
            g2copy(r).start()

    def g1copy(n):
        dz, lo, cnt = ((1, 0, 4), (-1, 0, 4), (2, 0, 2), (-2, 2, 2))[n]
        ref = gat.at[core, cls, pl.ds(lo, cnt)]
        return pltpu.make_async_remote_copy(
            src_ref=ref, dst_ref=ref, send_sem=s_ss, recv_sem=g1_rs.at[min(n, 2)],
            device_id=zdev(dz), device_id_type=MESH,
        )

    def gdcopy(dk):
        ref = gat.at[core, (cls + dk) % 4]
        return pltpu.make_async_remote_copy(
            src_ref=ref, dst_ref=ref, send_sem=s_ss, recv_sem=gd_rs.at[dk],
            device_id=dev(cc=1 - core), device_id_type=MESH,
        )

    def far_back():
        drain(r2r, g2_rs)
        for n in (2, 3, 0, 1):
            g1copy(n).start()
        gdcopy(0).start()
        prep(0, core, cls)

    order = ((core, 0), (1 - core, 0), (core, 3), (core, 1), (1 - core, 3), (1 - core, 1), (core, 2), (1 - core, 2))

    def take(n, dk):
        drain(gat.at[core, cls], g1_rs.at[{3: 0, 1: 1, 2: 2}[dk]])
        gdcopy(dk).start()
        prep(n, core, (cls + dk) % 4)
        mix(n - 1)

    def twin(n, dk, before=True):
        gdcopy(dk).wait_recv()
        prep(n, 1 - core, (cls + dk) % 4)
        if before:
            mix(n - 1)

    def prep(step, half, k):
        row = lax.broadcasted_iota(jnp.int32, (16, 256), 0)
        col = lax.broadcasted_iota(jnp.int32, (16, 256), 1) // 128
        pick = jnp.where(row == 8 * col, 1.0 / 64.0, 0.0).astype(BF)
        zero = jnp.zeros((128, 128), BF)
        for m in range(4):
            s = gat[half, k, m]
            a = s[0:64].astype(F32)
            n = lax.dot_general(s[64:80], pick, (((0,), (0,)), ((), ())), preferred_element_type=F32)
            at = 4 * step + m
            rhs[at, 0:64, 0:128] = jnp.where(lane, a, 0.0).astype(BF)
            rhs[at, 64:128, 0:128] = jnp.where(lane, 0.0, a).astype(BF)
            rhs[at, 128:256, 0:128] = zero
            rhs[at, 0:64, 128:256] = jnp.where(lane, n[0:64, 0:128], 0.0).astype(BF)
            rhs[at, 64:128, 128:256] = jnp.where(lane, 0.0, n[64:128, 0:128]).astype(BF)
            rhs[at, 128:192, 128:256] = jnp.where(lane, n[0:64, 128:256], 0.0).astype(BF)
            rhs[at, 192:256, 128:256] = jnp.where(lane, 0.0, n[64:128, 128:256]).astype(BF)

    def mix(step):
        half, dk = order[step]
        k = (cls + dk) % 4
        for m in range(4):
            r = pl.ds(pl.multiple_of((16 * half + 4 * m + k) * 128, 128), 128)
            w = rhs[4 * step + m]
            for u in range(4):
                t0 = pl.ds(u * T, T)
                f = qf[t0, r]
                g = jnp.dot(jnp.concatenate([f, f], axis=1), w, preferred_element_type=F32)
                mixed[t0, r] = (g[:, 0:128] / (g[:, 128:256] + 1e-3 / 64.0)).astype(BF)

    def rows(slot):
        return pl.ds(pl.multiple_of(slot * T, T), T)

    def cols(c):
        buf, lo, width = CHUNKS[c]
        return pl.ds(pl.multiple_of(quarter * (NC * CW) + buf * CW + lo, 128), width)

    def ocopy(c, slot, target):
        buf, lo, width = CHUNKS[c]
        return pltpu.make_async_remote_copy(
            src_ref=obuf.at[buf, rows(slot), pl.ds(lo, width)], dst_ref=out_ref.at[:, cols(c)],
            send_sem=o_ss, recv_sem=o_rs, device_id=target, device_id_type=MESH,
        )

    znear = {2: dev(zz=(z + 1) % 16, cc=0), 3: dev(zz=(z + 15) % 16, cc=1)}

    def part(c, r, k=pl.ds(0, D)):
        buf, lo, width = CHUNKS[c]
        return jnp.dot(mixed[r, k], wbuf[buf, k, lo : lo + width], preferred_element_type=F32)

    def put(c, r, value):
        buf, lo, width = CHUNKS[c]
        obuf[buf, r, lo : lo + width] = value.astype(BF)

    def own(c):
        buf, lo, width = CHUNKS[c]
        ocopy(c, sib, twin_core).start()
        out_ref[:, cols(c)] = obuf[buf, rows(me), lo : lo + width]

    def project(c):
        for first in (2, 0):
            r = pl.ds(first * T, 2 * T)
            put(c, r, part(c, r))
        ocopy(c, 2, znear[2]).start()
        ocopy(c, 3, znear[3]).start()
        own(c)

    def far_tokens(c, halves):
        for slot in (2, 3):
            r = pl.ds(slot * T, T)
            if halves:
                put(c, r, part(c, r, pl.ds(0, D // 2)) + part(c, r, pl.ds(D // 2, D // 2)))
                ocopy(c, slot, znear[slot]).start()
            else:
                put(c, r, part(c, r))
        if not halves:
            for slot in (2, 3):
                ocopy(c, slot, znear[slot]).start()

    def near_tokens(c):
        for slot in (0, 1):
            r = pl.ds(slot * T, T)
            put(c, r, part(c, r))
        own(c)

    def o_wait():
        drain(obuf.at[pl.ds(0, 3)], o_rs)

    def finish():
        drain(obuf.at[pl.ds(0, 3)], o_ss)
        drain(wbuf.at[0, pl.ds(0, 2480), :], s_ss)
        drain(wbuf.at[:, pl.ds(0, 3840), :], w_ss)
        drain(qbuf.at[pl.ds(0, 3)], q_ss)

    plan = [
        ("start", start),
        ("theirs", theirs),
        ("mine", mine),
        ("z_ready", z_ready),
        ("qlink0", lambda: qlink(0, 2)),
        ("chip_sum", chip_sum),
        ("qlink1", lambda: qlink(2, 6)),
        ("e1_0", lambda: e1(0)),
        ("far_ready", far_ready),
        ("e1_1", lambda: e1(1)),
        ("near_sum", near_sum),
        ("qlink2", lambda: qlink(6, 12)),
        ("e1_2", lambda: e1(2)),
        ("qf_me", lambda: qfeat(me, 0, QP)),
        ("e1_3", lambda: e1(3)),
        ("qsib", lambda: qwait(0, QP)),
        ("qf_sib", lambda: qfeat(sib, 0, QP)),
        ("far_sum", far_sum),
        ("qlink3", lambda: qlink(12, QP)),
        ("e3_0", lambda: e3(0)),
        ("qrelay1", lambda: qrelay(0)),
        ("qf_zs", lambda: qfeat(zs, 0, 8)),
        ("e3_1", lambda: e3(1)),
        ("e4a_0", lambda: e4(0, 0)),
        ("qtwin1", lambda: qwait(3, 8)),
        ("qf_tw", lambda: qfeat(zs2, 0, 8)),
        ("e4a_1", lambda: e4(1, 0)),
        ("e3_2", lambda: e3(2)),
        ("far_back", far_back),
        ("qrelay2", lambda: qrelay(1)),
        ("qf_zs2", lambda: qfeat(zs, 8, QP)),
        ("twin0", lambda: twin(1, 0, before=False)),
        ("e4b_0", lambda: e4(0, 1)),
        ("qtwin2", lambda: qwait(4, 8)),
        ("e3_3", lambda: e3(3)),
        ("qf_tw2", lambda: qfeat(zs2, 8, QP)),
        ("e4b_1", lambda: e4(1, 1)),
        ("mix0", lambda: mix(0)),
        ("e4a_2", lambda: e4(2, 0)),
        ("take3", lambda: take(2, 3)),
        ("take1", lambda: take(3, 1)),
        ("e4a_3", lambda: e4(3, 0)),
        ("twin3", lambda: twin(4, 3)),
        ("e4b_2", lambda: e4(2, 1)),
        ("twin1", lambda: twin(5, 1)),
        ("take2", lambda: take(6, 2)),
        ("twin2", lambda: twin(7, 2)),
        ("e4b_3", lambda: e4(3, 1)),
        ("mix7", lambda: mix(7)),
        ("e5_0", lambda: e5(0)),
        ("pr_0", lambda: project(0)),
        ("e5_1", lambda: e5(1)),
        ("pr_1", lambda: project(1)),
        ("e5_2", lambda: e5(2)),
        ("prf_2", lambda: far_tokens(2, False)),
        ("e5_3", lambda: e5(3)),
        ("prf_3", lambda: far_tokens(3, True)),
        ("prn_2", lambda: near_tokens(2)),
        ("prn_3", lambda: near_tokens(3)),
        ("o_wait", o_wait),
        ("finish", finish),
    ]
    for name, step in plan:
        step()


def shards(asked_for, offered, contents, out_weight):
    def view(a):
        return jnp.transpose(a, (0, 2, 3, 1)).reshape(D, T)

    dma = pltpu.SemaphoreType.DMA
    hbm = pl.BlockSpec(memory_space=pl.ANY)
    out = pl.pallas_call(
        kernel,
        out_shape=pltpu.VMEM((T, D), BF),
        in_specs=[hbm] * 4,
        out_specs=pl.BlockSpec(memory_space=pltpu.VMEM),
        scratch_shapes=[
            pltpu.VMEM((NC, D, CW), BF),
            pltpu.VMEM((4, D, T), BF),
            pltpu.VMEM((D, T), BF),
            pltpu.VMEM((D, T), BF),
            pltpu.VMEM((4 * T, D), BF),
            pltpu.VMEM((4, 4, SR, 128), F32),
            pltpu.VMEM((4, 4, SR, 128), BF),
            pltpu.VMEM((4, 4, SR, 128), BF),
            pltpu.VMEM((4, 4, SR, 128), BF),
            pltpu.VMEM((3, 4, SR, 128), BF),
            pltpu.VMEM((4, SR, 128), F32),
            pltpu.VMEM((4, SR, 128), BF),
            pltpu.VMEM((3, SR, 128), BF),
            pltpu.VMEM((2, 4, 4, SR, 128), BF),
            pltpu.VMEM((32, 256, 256), BF),
            pltpu.VMEM((4 * T, D), BF),
            pltpu.VMEM((NC, 4 * T, CW), BF),
            dma((NC + 3,)), dma, dma((NC, 5)), dma, dma((5,)), dma, dma, dma, dma, dma, dma((3,)), dma((4,)), dma, dma,
            *[pltpu.SemaphoreType.REGULAR] * 4,
        ],
        compiler_params=pltpu.CompilerParams(
            collective_id=0, has_side_effects=True, vmem_limit_bytes=56 * 1024 * 1024
        ),
        name="attend_project",
    )(view(asked_for), view(offered), view(contents), out_weight)
    return out.reshape(1, T, D)


def solution(mesh):
    in_specs = (
        P("batch", "ctx", None, None),
        P("batch", "ctx", None, None),
        P("batch", "ctx", None, None),
        P("batch", None),
    )
    return jax.shard_map(shards, mesh=mesh, in_specs=in_specs, out_specs=P("batch", "ctx", None), check_vma=False)
```
